32 devices in a mesh: grp: 4 (over y, x), bal: 8 (over z, core).
Axes of the slice: x: 2, y: 2, z: 4, core: 2. Of those that a mesh axis runs over, the one named last changes fastest.
Arguments:
- tracers: float32 [2, 64, 16, 2048], P(None, None, 'grp', 'bal'), may hold values from -6 to 6
- winds: bfloat16 [2, 64, 16, 2048], P(None, None, 'grp', 'bal'), may hold values from -16 to 16
- node_mass: float32 [16, 2048], P('grp', 'bal'), may hold values from 0.07 to 5.6
- column_cost: int32 [8, 1024], P('grp', 'bal'), may hold values from 1 to 3, as said below
- weight_in: bfloat16 [256, 1024], replicated, may hold values from -0.375 to 0.375
- weight_out: bfloat16 [1024, 256], replicated, may hold values from -0.1875 to 0.1875
Outputs:
- tracers_next: float32 [2, 64, 16, 2048], P(None, None, 'grp', 'bal')
- columns_out: bfloat16 [4, 64, 8, 1024], P(None, None, 'grp', 'bal')
The draws below stay inside these ranges and needn't reach their ends.
Inputs may be any that keep to these rules, and one draw needn't show every extreme that they name: `column_cost`: among the columns of one index of grp (rows 2 * g to 2 * g + 1 of all columns), exactly a quarter have cost 3 and exactly a quarter cost 2.
All inputs are finite; a program needn't handle non-finite values.
Results may differ from the reference program's by a relative error of at most 0.008.
Values may be sent and summed in bfloat16 or wider, within the bound.
A program may use at most 64 MiB of HBM per device.

```python
import math
import jax
import jax.numpy as jnp
from jax import lax

EX = 1
EY = 64
LEV = 64
HID = 1024
NEX = 4
NEY = 512
COLS = 256
N_GRP = 4
N_BAL = 8


def draw_column_cost(key, part):
    per_device = 4 * EX * EY
    members = per_device * N_BAL
    key_bias = jax.random.fold_in(key, 11)
    key_fine = jax.random.fold_in(key, 23)
    device_bias = jax.random.randint(key_bias, (N_GRP, N_BAL, 1), 0, 4)
    fine_bits = jax.random.randint(key_fine, (N_GRP, N_BAL, per_device), 0, 2048)
    position = jnp.arange(members, dtype=jnp.int32).reshape(1, N_BAL, per_device)
    scores = (device_bias * 2048 + fine_bits) * members + position
    flat_scores = scores.reshape(N_GRP, members)
    sorted_order = jnp.argsort(-flat_scores, axis=1)
    ranking = jnp.argsort(sorted_order, axis=1)
    costs_flat = jnp.where(ranking < members // 4, 3, jnp.where(ranking < members // 2, 2, 1)).astype(jnp.int32)
    blocks = costs_flat.reshape(N_GRP, N_BAL, 2 * EX, 2 * EY)
    return blocks.transpose(0, 2, 1, 3).reshape(N_GRP * 2 * EX, N_BAL * 2 * EY)


def draw_winds(key, part):
    layout = (2, LEV, 4 * NEX, 4 * NEY)
    key_sign = jax.random.fold_in(key, 101)
    key_size = jax.random.fold_in(key, 103)
    signs = jax.random.randint(key_sign, layout, 0, 2).astype(jnp.float32) * 2.0 - 1.0
    magnitude = jax.random.uniform(key_size, layout, jnp.float32, 10.0, 16.0)
    return (signs * magnitude).astype(jnp.bfloat16)


def draw_node_mass(key, part):
    key_flip = jax.random.fold_in(key, 201)
    key_elem = jax.random.fold_in(key, 203)
    key_node = jax.random.fold_in(key, 205)
    flip = jax.random.randint(key_flip, (), 0, 2)
    rows_idx = jnp.arange(NEX, dtype=jnp.int32)[:, None]
    cols_idx = jnp.arange(NEY, dtype=jnp.int32)[None, :]
    heavy = (rows_idx + cols_idx + flip) % 2 == 0
    spread = jax.random.uniform(key_elem, (NEX, NEY), jnp.float32, 0.0, 1.0)
    heavy_vals = 2.0 * jnp.exp(math.log(2.0) * spread)
    light_vals = 0.1 * jnp.exp(math.log(2.0) * spread)
    element_mass = jnp.where(heavy, heavy_vals, light_vals)
    expanded = jnp.repeat(jnp.repeat(element_mass, 4, axis=0), 4, axis=1)
    jitter = jnp.exp(jax.random.uniform(key_node, (4 * NEX, 4 * NEY), jnp.float32, math.log(0.7), math.log(1.4)))
    return (expanded * jitter).astype(jnp.float32)


def shard_levels(rng, extent, pieces, smallest, largest):
    factor_of = 1.0
    for dim, parts in pieces:
        steps = jax.random.uniform(jax.random.fold_in(jax.random.fold_in(rng, 6), dim), (parts,), jnp.float32, smallest / len(pieces), largest / len(pieces))
        factor_of = factor_of * jnp.repeat(jnp.exp(steps), extent[dim] // parts).reshape((-1,) + (1,) * (len(extent) - 1 - dim))
    return factor_of


def centred(own_key, dims, width, reach, shards=(), kind=jnp.bfloat16):
    level = shard_levels(own_key, dims, shards, -0.22, 0.18) if shards else 1.0
    values = jax.random.normal(own_key, dims, jnp.float32) * width * level
    return jnp.minimum(jnp.maximum(values, -reach), reach).astype(kind)


def setup_inputs(seed: int = 0) -> dict:
    keys = jax.random.split(jax.random.key(seed), 7)
    return {
        "tracers": centred(keys[0], (2, LEV, 4 * NEX, 4 * NEY), 1.0, 6.0, ((2, 4), (3, 8)), jnp.float32),
        "winds": draw_winds(jax.random.fold_in(keys[6], 71), 0),
        "node_mass": draw_node_mass(jax.random.fold_in(keys[6], 71), 0),
        "column_cost": draw_column_cost(jax.random.fold_in(keys[6], 71), 0),
        "weight_in": centred(keys[4], (4 * LEV, HID), (4 * LEV) ** -0.5, 0.375),
        "weight_out": centred(keys[5], (HID, 4 * LEV), HID ** -0.5, 0.1875),
    }


time_step = 0.02
remap_table = ((0.45, 0.4, 0.15, 0.0), (0.0, 0.15, 0.4, 0.45))
gll_points = (-1.0, -0.4472135954999579, 0.4472135954999579, 1.0)


def gll_matrix():
    matrix = []
    for row_idx in range(4):
        entries = []
        for col_idx in range(4):
            if row_idx == col_idx:
                running = 0.0
                for third_idx in range(4):
                    if third_idx != row_idx:
                        running += 1.0 / (gll_points[row_idx] - gll_points[third_idx])
                entries.append(2.0 * running)
            else:
                numerator = 1.0
                denominator = 1.0
                for third_idx in range(4):
                    if third_idx != row_idx:
                        numerator *= gll_points[row_idx] - gll_points[third_idx]
                    if third_idx != col_idx:
                        denominator *= gll_points[col_idx] - gll_points[third_idx]
                entries.append(2.0 * numerator / (denominator * (gll_points[row_idx] - gll_points[col_idx])))
        matrix.append(entries)
    return matrix


def derivatives(values):
    derivative = jnp.array(gll_matrix(), jnp.float32)
    layout = values.shape
    blocks_x = values.reshape(layout[:-2] + (layout[-2] // 4, 4, layout[-1]))
    along_x = jnp.einsum("ij,...ejy->...eiy", derivative, blocks_x, precision=lax.Precision.HIGHEST).reshape(layout)
    blocks_y = values.reshape(layout[:-1] + (layout[-1] // 4, 4))
    along_y = jnp.einsum("ij,...ej->...ei", derivative, blocks_y, precision=lax.Precision.HIGHEST).reshape(layout)
    return along_x, along_y


def tendency(tracer_vals, wind_vals):
    along_x, along_y = derivatives(tracer_vals)
    speeds = wind_vals.astype(jnp.float32)
    return -(speeds[0] * along_x + speeds[1] * along_y)


def assemble(values):
    layout = values.shape
    blocks = values.reshape(layout[:-2] + (layout[-2] // 4, 4, layout[-1]))
    first_edge = blocks[..., 0, :]
    last_edge = blocks[..., 3, :]
    new_first = first_edge + jnp.roll(last_edge, 1, axis=-2)
    new_last = last_edge + jnp.roll(first_edge, -1, axis=-2)
    blocks = jnp.concatenate([new_first[..., None, :], blocks[..., 1:3, :], new_last[..., None, :]], axis=-2)
    values = blocks.reshape(layout)
    blocks = values.reshape(layout[:-1] + (layout[-1] // 4, 4))
    first_edge = blocks[..., 0]
    last_edge = blocks[..., 3]
    new_first = first_edge + jnp.roll(last_edge, 1, axis=-1)
    new_last = last_edge + jnp.roll(first_edge, -1, axis=-1)
    blocks = jnp.concatenate([new_first[..., None], blocks[..., 1:3], new_last[..., None]], axis=-1)
    return blocks.reshape(layout)


def remap_columns(stacked):
    weights_table = jnp.array(remap_table, jnp.float32)
    layout = stacked.shape
    blocks = stacked.reshape(layout[:-2] + (layout[-2] // 4, 4, layout[-1] // 4, 4))
    cell_values = jnp.einsum("pa,qb,...xayb->...xpyq", weights_table, weights_table, blocks, precision=lax.Precision.HIGHEST)
    return cell_values.reshape(layout[:-2] + (layout[-2] // 2, layout[-1] // 2))


def network_step(column_state, weight_in, weight_out):
    hidden = jax.nn.gelu(jnp.dot(column_state.astype(jnp.bfloat16), weight_in, preferred_element_type=jnp.float32)).astype(jnp.bfloat16)
    return column_state + jnp.dot(hidden, weight_out, preferred_element_type=jnp.float32)


def blockwise(block_rows, weight_in, weight_out):
    blocks_count = block_rows.shape[0] // COLS
    mapped = lax.map(lambda one_block: network_step(one_block, weight_in, weight_out), block_rows.reshape(blocks_count, COLS, block_rows.shape[1]))
    return mapped.reshape(block_rows.shape)


def reference(tracers, winds, node_mass, column_cost, weight_in, weight_out):
    assembled = assemble(node_mass)

    def one_level(level_pair):
        tracer_level, wind_level = level_pair
        summed = assemble(tendency(tracer_level, wind_level) * node_mass)
        updated = tracer_level + time_step * (summed / assembled)
        stacked = jnp.concatenate([updated, wind_level.astype(jnp.float32)], axis=0)
        return updated, remap_columns(stacked).astype(jnp.bfloat16)

    by_level = (jnp.moveaxis(tracers, 1, 0), jnp.moveaxis(winds, 1, 0))
    updated, cell_values = lax.map(one_level, by_level)
    tracers_next = jnp.moveaxis(updated, 0, 1)
    cell_values = jnp.moveaxis(cell_values, 0, 1)
    features = cell_values.shape[0] * cell_values.shape[1]
    column_state = cell_values.reshape(features, -1).T.astype(jnp.float32)
    flat_cost = column_cost.reshape(-1)
    sorted_order = jnp.argsort(3 - flat_cost, stable=True)
    inverse = jnp.argsort(sorted_order, stable=True)
    column_state = column_state[sorted_order]
    everything = column_state.shape[0]
    for fraction in (1, 2, 4):
        leading = everything // fraction
        column_state = jnp.concatenate([blockwise(column_state[:leading], weight_in, weight_out), column_state[leading:]], axis=0)
    column_state = column_state[inverse].astype(jnp.bfloat16)
    columns_out = column_state.T.reshape(cell_values.shape)
    return tracers_next, columns_out
```

```python
import functools

import jax
import jax.numpy as jnp
import numpy as np
from jax import lax
from jax.experimental import pallas as pl
from jax.experimental.pallas import tpu as pltpu
from jax.sharding import PartitionSpec as P

MESH = pl.DeviceIdType.MESH
time_step = 0.02
remap_ints = ((9.0, 8.0, 3.0, 0.0), (0.0, 3.0, 8.0, 9.0))
gll_points = (-1.0, -0.4472135954999579, 0.4472135954999579, 1.0)

DIRS = ((1, 0), (-1, 0), (0, 1), (0, -1), (1, 1), (1, -1), (-1, 1), (-1, -1))
FROM_UP, FROM_DOWN, FROM_LEFT, FROM_RIGHT = 0, 1, 2, 3
FROM_UL, FROM_UR, FROM_DL, FROM_DR = 4, 5, 6, 7


def gll_matrix():
    points = gll_points
    matrix = np.zeros((4, 4))
    for i in range(4):
        for j in range(4):
            if i == j:
                matrix[i, i] = 2.0 * sum(
                    1.0 / (points[i] - points[k]) for k in range(4) if k != i
                )
            else:
                num = den = 1.0
                for k in range(4):
                    if k != i:
                        num *= points[i] - points[k]
                    if k != j:
                        den *= points[j] - points[k]
                matrix[i, j] = 2.0 * num / (den * (points[i] - points[j]))
    return matrix


def constants(across):
    elements, half = across // 4, across // 2
    eye = np.eye(elements)
    along = np.kron(eye, gll_matrix().T).astype(np.float32)
    high = along.astype(jnp.bfloat16)
    low = (along - high.astype(np.float32)).astype(jnp.bfloat16)
    remap = np.kron(eye, np.array(remap_ints).T).astype(jnp.bfloat16)
    pick = np.zeros((4, 8, across), np.float32)
    place = np.zeros((16, 5 * across), np.float32)
    for a in range(4):
        pick[a, a, 0] = 1.0
        pick[a, 4 + a, across - 1] = 1.0
        for part in range(2):
            place[8 * part + a, a * across] = 1.0
            place[8 * part + 4 + a, a * across + across - 1] = 1.0
            for p in range(2):
                first = 4 * across + p * half
                place[8 * part + a, first] = remap_ints[p][a] * remap_ints[0][0]
                place[8 * part + 4 + a, first + half - 1] = remap_ints[p][a] * remap_ints[1][3]
    return high, low, remap, pick.astype(jnp.bfloat16), place.astype(jnp.bfloat16)


def dot(a, b):
    return jnp.dot(a, b, preferred_element_type=jnp.float32)


def split(value):
    high = value.astype(jnp.bfloat16)
    return high, (value - high.astype(jnp.float32)).astype(jnp.bfloat16)


def kernel(
    sizes,
    tracers_hbm, winds_hbm, mass_hbm,
    dhigh_hbm, dlow_hbm, remap_hbm, pick_hbm, place_hbm, win_hbm, wout_hbm,
    next_ref, start_ref, win_t_ref, wout_t_ref,
    tracers_ref, winds_ref, mass_ref,
    dhigh_ref, dlow_ref, remap_ref, pick_ref, place_ref, win_ref, wout_ref,
    weighted, cells_ref, rows_out, rows_in, corners_out, ends_out, ends_in,
    mass_in, local_sem, send_sem, recv_sem, ack_sem,
):
    n_grp, n_bal = sizes
    levels, across = winds_ref.shape[1], winds_ref.shape[3]
    grp, bal = lax.axis_index("grp"), lax.axis_index("bal")
    is_first, is_last = bal == 0, bal == n_bal - 1

    def peer(i):
        dg, db = DIRS[i]
        return (lax.rem(grp + dg + n_grp, n_grp), lax.rem(bal + db + n_bal, n_bal))

    to_left = [i for i in range(8) if DIRS[i][1] == -1]
    to_right = [i for i in range(8) if DIRS[i][1] == 1]

    barrier = pltpu.get_barrier_semaphore()

    def greet(i):
        pl.semaphore_signal(barrier, inc=1, device_id=peer(i), device_id_type=MESH)

    for i in range(2):
        greet(i)

    @pl.when(is_first)
    def _():
        for i in to_left:
            greet(i)

    @pl.when(jnp.logical_not(is_last))
    def _():
        for i in to_right:
            greet(i)

    def load(src, dst, slot):
        copy = pltpu.make_async_copy(src, dst, local_sem.at[slot])
        copy.start()
        return copy

    load_mass = load(mass_hbm, mass_ref, 7)
    load_rows = [load(tracers_hbm.at[:, :, a, :], tracers_ref.at[a], a) for a in range(4)]
    load_winds = load(winds_hbm, winds_ref, 6)
    load_high = load(dhigh_hbm, dhigh_ref, 4)
    load_low = load(dlow_hbm, dlow_ref, 5)
    load_pick = load(pick_hbm, pick_ref, 8)
    load_remap = load(remap_hbm, remap_ref, 9)
    load_place = load(place_hbm, place_ref, 10)

    load_mass.wait()
    mass_ends = jnp.concatenate(
        [
            jnp.broadcast_to(mass_ref[a : a + 1, lane : lane + 1], (1, 2 * levels))
            for lane in (0, across - 1) for a in range(4)
        ],
        axis=0,
    )
    corners_out[8:16, :] = mass_ends
    ends_out[8:16, :] = mass_ends
    for copy in (load_high, load_low, load_winds, *load_rows):
        copy.wait()

    def tracer_row(a):
        return tracers_ref[a].reshape(2 * levels, across)

    derivative = gll_matrix()

    def weigh(a):
        here = tracer_row(a)
        high, low = split(here)
        along_y = dot(high, dhigh_ref[...]) + dot(low, dhigh_ref[...]) + dot(high, dlow_ref[...])
        along_x = sum(float(derivative[a, c]) * tracer_row(c) for c in range(4))
        first = winds_ref[0, :, a, :].astype(jnp.float32)
        second = winds_ref[1, :, a, :].astype(jnp.float32)
        mass = mass_ref[a : a + 1, :]
        first, second = first * mass, second * mass
        for k in range(2):
            part = slice(k * levels, (k + 1) * levels)
            weighted[a, part, :] = -(first * along_x[part] + second * along_y[part])

    def picked(a):
        return lax.dot_general(
            pick_ref[a], weighted[a].astype(jnp.bfloat16), (((1,), (1,)), ((), ())),
            preferred_element_type=jnp.float32,
        )

    for a in (0, 3):
        weigh(a)
    rows_out[0] = weighted[3].astype(jnp.bfloat16)
    rows_out[1] = weighted[0].astype(jnp.bfloat16)
    load_pick.wait()
    corners = picked(0) + picked(3)
    corners_out[0:8, :] = corners

    def remote(src, dst, slot, i):
        return pltpu.make_async_remote_copy(
            src_ref=src, dst_ref=dst, send_sem=send_sem.at[slot], recv_sem=recv_sem.at[slot],
            device_id=peer(i), device_id_type=MESH,
        )

    mass_copies = [remote(mass_ref, mass_in.at[i], i, i) for i in range(2)]
    row_copies = [remote(rows_out.at[i], rows_in.at[i], 2 + i, i) for i in range(2)]
    end_copies = [
        remote(ends_out if i in (2, 3) else corners_out, ends_in.at[i], 4 + i, i) for i in range(8)
    ]

    before = jnp.where(bal > 0, 3, 0) + jnp.where(is_last, 3, 0)
    pl.semaphore_wait(barrier, 2 + before)

    def answer(slot, i):
        pl.semaphore_signal(ack_sem.at[slot], inc=1, device_id=peer(i), device_id_type=MESH)

    @pl.when(jnp.logical_not(is_first))
    def _():
        for i in to_left:
            answer(1, i)
        for i in to_left:
            if i > 3:
                end_copies[i].start()

    @pl.when(is_last)
    def _():
        for i in to_right:
            answer(0, i)
        for i in to_right:
            if i > 3:
                end_copies[i].start()

    for copy in (*mass_copies, *row_copies, *end_copies[:2]):
        copy.start()

    for a in (1, 2):
        weigh(a)
    ends_out[0:8, :] = corners + (picked(1) + picked(2))

    @pl.when(jnp.logical_not(is_first))
    def _():
        end_copies[3].start()

    @pl.when(is_last)
    def _():
        end_copies[2].start()

    @pl.when(jnp.logical_not(is_last))
    def _():
        pl.semaphore_wait(ack_sem.at[1], 3)
        for i in to_right:
            end_copies[i].start()

    load_win = load(win_hbm, win_ref, 11)
    load_wout = load(wout_hbm, wout_ref, 12)

    lane = lax.broadcasted_iota(jnp.int32, (1, across), 1)
    takes_before = (lane % 4 == 0) & (lane > 0)
    takes_after = (lane % 4 == 3) & (lane < across - 1)
    inside = (lane > 0) & (lane < across - 1)

    half = across // 2
    load_remap.wait()

    def cells(mixed):
        high, low = split(mixed)
        return dot(high, remap_ref[...]) + dot(low, remap_ref[...])

    for p in range(2):
        parts = [
            sum(
                remap_ints[p][a] * winds_ref[k, :, a, :].astype(jnp.float32)
                for a in range(4) if remap_ints[p][a]
            )
            for k in range(2)
        ]
        start_ref[2 * levels :, p * half : (p + 1) * half] = (
            cells(jnp.concatenate(parts, axis=0)) * (1.0 / 400.0)
        ).astype(jnp.bfloat16)

    load_win.wait()
    win_t_ref[...] = win_ref[...].T
    load_wout.wait()
    wout_t_ref[...] = wout_ref[...].T

    for copy in mass_copies:
        copy.wait_recv()
    own = [mass_ref[a : a + 1, :] for a in range(4)]
    own[0] = own[0] + mass_in[FROM_UP, 3:4, :]
    own[3] = own[3] + mass_in[FROM_DOWN, 0:1, :]

    def joined(value):
        earlier = pltpu.roll(value, 1, 1)
        later = pltpu.roll(value, across - 1, 1)
        return value + jnp.where(takes_before, earlier, jnp.where(takes_after, later, 0.0))

    scales = [jnp.where(inside, time_step / joined(own[a]), 0.0) for a in range(4)]

    load_place.wait()

    @pl.when(is_first)
    def _():
        pl.semaphore_wait(ack_sem.at[0], 3)
        for i in to_left:
            end_copies[i].start()

    for copy in row_copies:
        copy.wait_recv()
    mixed = [None, None]
    for a in range(4):
        value = weighted[a]
        if a == 0:
            value = value + rows_in[FROM_UP].astype(jnp.float32)
        if a == 3:
            value = value + rows_in[FROM_DOWN].astype(jnp.float32)
        updated = tracer_row(a) + scales[a] * joined(value)
        next_ref[a] = updated
        for p in range(2):
            if remap_ints[p][a]:
                term = remap_ints[p][a] * updated
                mixed[p] = term if mixed[p] is None else mixed[p] + term
    for p in range(2):
        cells_ref[:, p * half : (p + 1) * half] = cells(mixed[p])

    for copy in end_copies:
        copy.wait_recv()

    def assembled(mine, first):
        def row(i, r):
            return ends_in[i, first + r : first + r + 1, :]

        lines = []
        for side, lateral, upper, lower in (
            (0, FROM_LEFT, FROM_UL, FROM_DL), (1, FROM_RIGHT, FROM_UR, FROM_DR)
        ):
            near, far = 4 * side, 4 - 4 * side
            for a in range(4):
                line = mine[near + a : near + a + 1, :] + row(lateral, far + a)
                if a == 0:
                    line = line + (row(FROM_UP, near + 3) + row(upper, far + 3))
                if a == 3:
                    line = line + (row(FROM_DOWN, near) + row(lower, far))
                lines.append(line)
        return jnp.concatenate(lines, axis=0)

    change = assembled(ends_out[0:8, :], 0) * (time_step / assembled(ends_out[8:16, :], 8))
    high = change.astype(jnp.bfloat16).astype(jnp.float32)
    parts = jnp.concatenate([high, change - high], axis=0).T.astype(jnp.bfloat16)
    final = cells_ref[...] + dot(parts, place_ref[:, 4 * across :])
    start_ref[0 : 2 * levels, :] = (final * (1.0 / 400.0)).astype(jnp.bfloat16)
    for a in range(4):
        next_ref[a] = next_ref[a] + dot(parts, place_ref[:, a * across : (a + 1) * across])

    for copy in (*mass_copies, *row_copies, *end_copies):
        copy.wait_send()


def doubled_gelu(value):
    inner = value * (0.7978845608028654 + 0.035677408136300125 * (value * value))
    return value + value * jnp.tanh(inner)


def columns_kernel(
    rows_ref, start_ref, cost_hbm, win_ref, wout_ref, next_hbm, cols_ref, cost_ref, load_sem, store_sem
):
    load_cost = pltpu.make_async_copy(cost_hbm, cost_ref, load_sem)
    load_cost.start()
    levels = next_hbm.shape[1]
    stores = [
        pltpu.make_async_copy(
            rows_ref.at[a, pl.ds(k * levels, levels), :], next_hbm.at[k, :, a, :], store_sem.at[a, k]
        )
        for a in range(4) for k in range(2)
    ]
    for copy in stores:
        copy.start()
    hidden_size, features = win_ref.shape
    half = cost_ref.shape[1]
    chunk = hidden_size // 4
    current = start_ref[...].astype(jnp.float32)
    for step in range(3):
        inputs = current.astype(jnp.bfloat16)
        change = None
        for c in range(4):
            part = slice(c * chunk, (c + 1) * chunk)
            hidden = doubled_gelu(dot(win_ref[part, :], inputs)).astype(jnp.bfloat16)
            term = dot(wout_ref[:, part], hidden)
            change = term if change is None else change + term
        if step == 0:
            load_cost.wait()
            cost = jnp.concatenate([cost_ref[0:1, :], cost_ref[1:2, :]], axis=1)
        current = current + jnp.where(cost > step, 0.5, 0.0) * change
    cols_ref[...] = jnp.stack([current[:, :half], current[:, half:]], axis=1).astype(jnp.bfloat16)
    for copy in stores:
        copy.wait()


def shards(sizes, tracers, winds, node_mass, column_cost, weight_in, weight_out):
    levels, extent, across = tracers.shape[1:]
    features, hidden = weight_in.shape
    channels = 2 * levels
    vmem = pl.BlockSpec(memory_space=pltpu.VMEM)
    hbm = pl.BlockSpec(memory_space=pltpu.HBM)
    f32, bf16 = jnp.float32, jnp.bfloat16
    rows = (extent, channels, across)
    tables = constants(across)
    columns = column_cost.size
    operands = (tracers, winds, node_mass, *map(jnp.asarray, tables), weight_in, weight_out)
    next_rows, start, win_t, wout_t = pl.pallas_call(
        functools.partial(kernel, sizes),
        out_shape=(
            jax.ShapeDtypeStruct(rows, f32),
            jax.ShapeDtypeStruct((features, columns), bf16),
            jax.ShapeDtypeStruct((hidden, features), bf16),
            jax.ShapeDtypeStruct((features, hidden), bf16),
        ),
        in_specs=[hbm] * 10,
        out_specs=(vmem,) * 4,
        scratch_shapes=[
            pltpu.VMEM((extent, 2, levels, across), f32),
            pltpu.VMEM(winds.shape, bf16),
            pltpu.VMEM(node_mass.shape, f32),
            *[pltpu.VMEM(table.shape, bf16) for table in tables],
            pltpu.VMEM(weight_in.shape, bf16),
            pltpu.VMEM(weight_out.shape, bf16),
            pltpu.VMEM(rows, f32),
            pltpu.VMEM((channels, across), f32),
            pltpu.VMEM((2, channels, across), bf16),
            pltpu.VMEM((2, channels, across), bf16),
            pltpu.VMEM((16, channels), f32),
            pltpu.VMEM((16, channels), f32),
            pltpu.VMEM((8, 16, channels), f32),
            pltpu.VMEM((2, extent, across), f32),
            pltpu.SemaphoreType.DMA((13,)),
            pltpu.SemaphoreType.DMA((12,)),
            pltpu.SemaphoreType.DMA((12,)),
            pltpu.SemaphoreType.REGULAR((2,)),
        ],
        compiler_params=pltpu.CompilerParams(
            collective_id=0, has_side_effects=True, vmem_limit_bytes=24 * 2**20
        ),
        cost_estimate=pl.CostEstimate(
            flops=10**9, bytes_accessed=4 * 2**20, transcendentals=0
        ),
    )(*(pltpu.with_memory_space_constraint(x, pltpu.HBM) for x in operands))
    tracers_next, cols = pl.pallas_call(
        columns_kernel,
        out_shape=(
            jax.ShapeDtypeStruct(tracers.shape, f32),
            jax.ShapeDtypeStruct((features, 2, across // 2), bf16),
        ),
        in_specs=[vmem, vmem, hbm, vmem, vmem],
        out_specs=(hbm, vmem),
        scratch_shapes=[
            pltpu.VMEM(column_cost.shape, column_cost.dtype),
            pltpu.SemaphoreType.DMA,
            pltpu.SemaphoreType.DMA((4, 2)),
        ],
        compiler_params=pltpu.CompilerParams(vmem_limit_bytes=24 * 2**20),
    )(next_rows, start, pltpu.with_memory_space_constraint(column_cost, pltpu.HBM), win_t, wout_t)
    return tracers_next, cols.reshape(4, levels, 2, across // 2)


def solution(mesh):
    grid = P(None, None, "grp", "bal")
    flat = P("grp", "bal")
    sizes = (mesh.shape["grp"], mesh.shape["bal"])
    return jax.shard_map(
        functools.partial(shards, sizes),
        mesh=mesh,
        in_specs=(grid, grid, flat, flat, P(), P()),
        out_specs=(grid, grid),
        check_vma=False,
    )
```

```python
import functools

import jax
import jax.numpy as jnp
import numpy as np
from jax import lax
from jax.experimental import pallas as pl
from jax.experimental.pallas import tpu as pltpu
from jax.sharding import PartitionSpec as P

MESH = pl.DeviceIdType.MESH
time_step = 0.02
remap_ints = ((9.0, 8.0, 3.0, 0.0), (0.0, 3.0, 8.0, 9.0))
gll_points = (-1.0, -0.4472135954999579, 0.4472135954999579, 1.0)

DIRS = ((1, 0), (-1, 0), (0, 1), (0, -1), (1, 1), (1, -1), (-1, 1), (-1, -1))
FROM_UP, FROM_DOWN, FROM_LEFT, FROM_RIGHT = 0, 1, 2, 3
FROM_UL, FROM_UR, FROM_DL, FROM_DR = 4, 5, 6, 7


def gll_matrix():
    points = gll_points
    matrix = np.zeros((4, 4))
    for i in range(4):
        for j in range(4):
            if i == j:
                matrix[i, i] = 2.0 * sum(
                    1.0 / (points[i] - points[k]) for k in range(4) if k != i
                )
            else:
                num = den = 1.0
                for k in range(4):
                    if k != i:
                        num *= points[i] - points[k]
                    if k != j:
                        den *= points[j] - points[k]
                matrix[i, j] = 2.0 * num / (den * (points[i] - points[j]))
    return matrix


def constants(across):
    elements, half = across // 4, across // 2
    eye = np.eye(elements)
    along = np.kron(eye, gll_matrix().T).astype(np.float32)
    high = along.astype(jnp.bfloat16)
    low = (along - high.astype(np.float32)).astype(jnp.bfloat16)
    remap = np.kron(eye, np.array(remap_ints).T).astype(jnp.bfloat16)
    pick = np.zeros((4, 8, across), np.float32)
    place = np.zeros((16, 5 * across), np.float32)
    for a in range(4):
        pick[a, a, 0] = 1.0
        pick[a, 4 + a, across - 1] = 1.0
        for part in range(2):
            place[8 * part + a, a * across] = 1.0
            place[8 * part + 4 + a, a * across + across - 1] = 1.0
            for p in range(2):
                first = 4 * across + p * half
                place[8 * part + a, first] = remap_ints[p][a] * remap_ints[0][0]
                place[8 * part + 4 + a, first + half - 1] = remap_ints[p][a] * remap_ints[1][3]
    return high, low, remap, pick.astype(jnp.bfloat16), place.astype(jnp.bfloat16)


def dot(a, b):
    return jnp.dot(a, b, preferred_element_type=jnp.float32)


def split(value):
    high = value.astype(jnp.bfloat16)
    return high, (value - high.astype(jnp.float32)).astype(jnp.bfloat16)


def kernel(
    sizes,
    tracers_hbm, winds_hbm, mass_hbm,
    dhigh_hbm, dlow_hbm, remap_hbm, pick_hbm, place_hbm, win_hbm, wout_hbm, cost_hbm,
    next_ref, start_ref, win_t_ref, wout_t_ref, cost_out_ref,
    tracers_ref, winds_ref, mass_ref,
    dhigh_ref, dlow_ref, remap_ref, pick_ref, place_ref, win_ref, wout_ref, cost_ref,
    weighted, cells_ref, rows_out, rows_in, corners_out, corners_in, sides_out, sides_in,
    mass_out, mass_in, local_sem, send_sem, recv_sem, ack_sem,
):
    n_grp, n_bal = sizes
    levels, across = winds_ref.shape[1], winds_ref.shape[3]
    grp, bal = lax.axis_index("grp"), lax.axis_index("bal")
    is_first, is_last = bal == 0, bal == n_bal - 1

    def peer(i):
        dg, db = DIRS[i]
        return (lax.rem(grp + dg + n_grp, n_grp), lax.rem(bal + db + n_bal, n_bal))

    to_left = [i for i in range(8) if DIRS[i][1] == -1]
    to_right = [i for i in range(8) if DIRS[i][1] == 1]

    def load(src, dst, slot):
        copy = pltpu.make_async_copy(src, dst, local_sem.at[slot])
        copy.start()
        return copy

    load_mass = load(mass_hbm, mass_ref, 7)
    load_rows = [load(tracers_hbm.at[:, :, a, :], tracers_ref.at[a], a) for a in range(4)]
    load_winds = load(winds_hbm, winds_ref, 6)
    load_high = load(dhigh_hbm, dhigh_ref, 4)
    load_low = load(dlow_hbm, dlow_ref, 5)
    load_pick = load(pick_hbm, pick_ref, 8)
    load_remap = load(remap_hbm, remap_ref, 9)
    load_place = load(place_hbm, place_ref, 10)

    barrier = pltpu.get_barrier_semaphore()

    def greet(i):
        pl.semaphore_signal(barrier, inc=1, device_id=peer(i), device_id_type=MESH)

    for i in range(2):
        greet(i)

    @pl.when(is_first)
    def _():
        for i in to_left:
            greet(i)

    @pl.when(jnp.logical_not(is_last))
    def _():
        for i in to_right:
            greet(i)

    load_mass.wait()

    def outermost(rows):
        return [
            jnp.broadcast_to(rows[a][:, lane : lane + 1], (1, 2 * levels))
            for lane in (0, across - 1) for a in range(4)
        ]

    own = [mass_ref[a : a + 1, :] for a in range(4)]
    mass_out[0] = own[3]
    mass_out[1] = own[0]
    mass_ends = outermost(own)
    for side in range(2):
        sides_out[side, 4:8, :] = jnp.concatenate(mass_ends[4 * side : 4 * side + 4], axis=0)
    for copy in (load_high, load_low, load_winds, *load_rows):
        copy.wait()

    def tracer_row(a):
        return tracers_ref[a].reshape(2 * levels, across)

    derivative = gll_matrix()

    def weigh(a):
        here = tracer_row(a)
        high, low = split(here)
        along_y = dot(high, dhigh_ref[...]) + dot(low, dhigh_ref[...]) + dot(high, dlow_ref[...])
        along_x = sum(float(derivative[a, c]) * tracer_row(c) for c in range(4))
        first = winds_ref[0, :, a, :].astype(jnp.float32)
        second = winds_ref[1, :, a, :].astype(jnp.float32)
        mass = mass_ref[a : a + 1, :]
        first, second = first * mass, second * mass
        for k in range(2):
            part = slice(k * levels, (k + 1) * levels)
            weighted[a, part, :] = -(first * along_x[part] + second * along_y[part])

    def picks(a, value):
        return lax.dot_general(
            pick_ref[a], value, (((1,), (1,)), ((), ())), preferred_element_type=jnp.float32
        )

    def picked(a):
        return picks(a, weighted[a].astype(jnp.bfloat16))

    for a in (0, 3):
        weigh(a)
    rows_out[0] = weighted[3].astype(jnp.bfloat16)
    rows_out[1] = weighted[0].astype(jnp.bfloat16)
    load_pick.wait()
    corners = picked(0) + picked(3)
    for c, line in enumerate((7, 3, 4, 0)):
        corners_out[c] = jnp.concatenate([corners[line : line + 1, :], mass_ends[line]], axis=0)

    def remote(src, dst, slot, i):
        return pltpu.make_async_remote_copy(
            src_ref=src, dst_ref=dst, send_sem=send_sem.at[slot], recv_sem=recv_sem.at[slot],
            device_id=peer(i), device_id_type=MESH,
        )

    mass_copies = [remote(mass_out.at[i], mass_in.at[i], i, i) for i in range(2)]
    row_copies = [remote(rows_out.at[i], rows_in.at[i], 2 + i, i) for i in range(2)]
    end_copies = {
        2: remote(sides_out.at[1], sides_in.at[0], 4, 2),
        3: remote(sides_out.at[0], sides_in.at[1], 5, 3),
        **{4 + c: remote(corners_out.at[c], corners_in.at[c], 6 + c, 4 + c) for c in range(4)},
    }

    before = jnp.where(bal > 0, 3, 0) + jnp.where(is_last, 3, 0)
    pl.semaphore_wait(barrier, 2 + before)

    def answer(slot, i):
        pl.semaphore_signal(ack_sem.at[slot], inc=1, device_id=peer(i), device_id_type=MESH)

    @pl.when(is_last)
    def _():
        for i in to_right:
            if i > 3:
                end_copies[i].start()
        for i in to_right:
            answer(0, i)

    @pl.when(jnp.logical_not(is_first))
    def _():
        for i in to_left:
            if i > 3:
                end_copies[i].start()
        for i in to_left:
            answer(1, i)

    for copy in (*mass_copies, *row_copies):
        copy.start()

    for a in (1, 2):
        weigh(a)
    ends = corners + (picked(1) + picked(2))
    for side in range(2):
        sides_out[side, 0:4, :] = ends[4 * side : 4 * side + 4, :]

    @pl.when(jnp.logical_not(is_first))
    def _():
        end_copies[3].start()

    @pl.when(is_last)
    def _():
        end_copies[2].start()

    @pl.when(jnp.logical_not(is_last))
    def _():
        pl.semaphore_wait(ack_sem.at[1], 3)
        for i in to_right:
            end_copies[i].start()

    load_win = load(win_hbm, win_ref, 11)
    load_wout = load(wout_hbm, wout_ref, 12)
    load_cost = load(cost_hbm, cost_ref, 13)

    lane = lax.broadcasted_iota(jnp.int32, (1, across), 1)
    takes_before = (lane % 4 == 0) & (lane > 0)
    takes_after = (lane % 4 == 3) & (lane < across - 1)
    inside = (lane > 0) & (lane < across - 1)

    half = across // 2
    load_remap.wait()

    def cells(mixed):
        high, low = split(mixed)
        return dot(high, remap_ref[...]) + dot(low, remap_ref[...])

    for p in range(2):
        parts = [
            sum(
                remap_ints[p][a] * winds_ref[k, :, a, :].astype(jnp.float32)
                for a in range(4) if remap_ints[p][a]
            )
            for k in range(2)
        ]
        start_ref[2 * levels :, p * half : (p + 1) * half] = (
            cells(jnp.concatenate(parts, axis=0)) * (1.0 / 400.0)
        ).astype(jnp.bfloat16)

    load_win.wait()
    win_t_ref[...] = win_ref[...].T
    load_wout.wait()
    wout_t_ref[...] = wout_ref[...].T
    load_cost.wait()
    cost_out_ref[...] = jnp.concatenate([cost_ref[0:1, :], cost_ref[1:2, :]], axis=1)

    for copy in mass_copies:
        copy.wait_recv()
    own[0] = own[0] + mass_in[FROM_UP]
    own[3] = own[3] + mass_in[FROM_DOWN]
    mass_ends = jnp.concatenate(outermost(own), axis=0)

    def joined(value):
        earlier = pltpu.roll(value, 1, 1)
        later = pltpu.roll(value, across - 1, 1)
        return value + jnp.where(takes_before, earlier, jnp.where(takes_after, later, 0.0))

    scales = [jnp.where(inside, time_step / joined(own[a]), 0.0) for a in range(4)]

    load_place.wait()

    @pl.when(is_first)
    def _():
        pl.semaphore_wait(ack_sem.at[0], 3)
        for i in to_left:
            end_copies[i].start()

    for copy in row_copies:
        copy.wait_recv()
    mixed = [None, None]
    for a in range(4):
        value = weighted[a]
        if a == 0:
            value = value + rows_in[FROM_UP].astype(jnp.float32)
        if a == 3:
            value = value + rows_in[FROM_DOWN].astype(jnp.float32)
        updated = tracer_row(a) + scales[a] * joined(value)
        next_ref[a] = updated
        for p in range(2):
            if remap_ints[p][a]:
                term = remap_ints[p][a] * updated
                mixed[p] = term if mixed[p] is None else mixed[p] + term
    ends = ends + (picks(0, rows_in[FROM_UP]) + picks(3, rows_in[FROM_DOWN]))
    for p in range(2):
        cells_ref[:, p * half : (p + 1) * half] = cells(mixed[p])

    for copy in end_copies.values():
        copy.wait_recv()

    def assembled(mine, first, line):
        none = jnp.zeros((2, 2 * levels), jnp.float32)
        upper_left, upper_right, lower_left, lower_right = (
            corners_in[i - 4, line : line + 1, :] for i in (FROM_UL, FROM_UR, FROM_DL, FROM_DR)
        )
        sides = jnp.concatenate([sides_in[side, first : first + 4, :] for side in range(2)], axis=0)
        diagonal = jnp.concatenate(
            [upper_left, none, lower_left, upper_right, none, lower_right], axis=0
        )
        return mine + (sides + diagonal)

    change = assembled(ends, 0, 0) * (time_step / assembled(mass_ends, 4, 1))
    high = change.astype(jnp.bfloat16).astype(jnp.float32)
    parts = jnp.concatenate([high, change - high], axis=0).T.astype(jnp.bfloat16)
    final = cells_ref[...] + dot(parts, place_ref[:, 4 * across :])
    start_ref[0 : 2 * levels, :] = (final * (1.0 / 400.0)).astype(jnp.bfloat16)
    for a in range(4):
        next_ref[a] = next_ref[a] + dot(parts, place_ref[:, a * across : (a + 1) * across])

    for copy in (*mass_copies, *row_copies, *end_copies.values()):
        copy.wait_send()


def doubled_gelu(value):
    inner = value * (0.7978845608028654 + 0.035677408136300125 * (value * value))
    return value + value * jnp.tanh(inner)


def columns_kernel(
    rows_ref, start_ref, win_ref, wout_ref, cost_ref, next_hbm, cols_ref, state_ref, paired_ref, store_sem
):
    levels = next_hbm.shape[1]
    stores = [
        pltpu.make_async_copy(
            rows_ref.at[a, pl.ds(k * levels, levels), :], next_hbm.at[k, :, a, :], store_sem.at[a, k]
        )
        for a in range(4) for k in range(2)
    ]
    for copy in stores:
        copy.start()
    hidden_size, features = win_ref.shape
    half = cols_ref.shape[1]
    chunk = hidden_size // 4
    state_ref[...] = start_ref[...].astype(jnp.float32)

    def substep(step, carry):
        inputs = state_ref[...].astype(jnp.bfloat16)
        change = None
        for c in range(4):
            part = slice(c * chunk, (c + 1) * chunk)
            hidden = doubled_gelu(dot(win_ref[part, :], inputs)).astype(jnp.bfloat16)
            term = dot(wout_ref[:, part], hidden)
            change = term if change is None else change + term
        state_ref[...] += jnp.where(cost_ref[...] > step, 0.5, 0.0) * change
        return carry

    lax.fori_loop(0, 3, substep, 0)
    current = state_ref[...]
    paired_ref[0::2, :] = current[:, :half]
    paired_ref[1::2, :] = current[:, half:]
    cols_ref[...] = paired_ref[...].astype(jnp.bfloat16)
    for copy in stores:
        copy.wait()


def shards(sizes, tracers, winds, node_mass, column_cost, weight_in, weight_out):
    levels, extent, across = tracers.shape[1:]
    features, hidden = weight_in.shape
    channels = 2 * levels
    vmem = pl.BlockSpec(memory_space=pltpu.VMEM)
    hbm = pl.BlockSpec(memory_space=pltpu.HBM)
    f32, bf16 = jnp.float32, jnp.bfloat16
    rows = (extent, channels, across)
    tables = constants(across)
    columns = column_cost.size
    operands = (tracers, winds, node_mass, *map(jnp.asarray, tables), weight_in, weight_out, column_cost)
    next_rows, start, win_t, wout_t, cost = pl.pallas_call(
        functools.partial(kernel, sizes),
        out_shape=(
            jax.ShapeDtypeStruct(rows, f32),
            jax.ShapeDtypeStruct((features, columns), bf16),
            jax.ShapeDtypeStruct((hidden, features), bf16),
            jax.ShapeDtypeStruct((features, hidden), bf16),
            jax.ShapeDtypeStruct((1, columns), column_cost.dtype),
        ),
        in_specs=[hbm] * 11,
        out_specs=(vmem,) * 5,
        scratch_shapes=[
            pltpu.VMEM((extent, 2, levels, across), f32),
            pltpu.VMEM(winds.shape, bf16),
            pltpu.VMEM(node_mass.shape, f32),
            *[pltpu.VMEM(table.shape, bf16) for table in tables],
            pltpu.VMEM(weight_in.shape, bf16),
            pltpu.VMEM(weight_out.shape, bf16),
            pltpu.VMEM(column_cost.shape, column_cost.dtype),
            pltpu.VMEM(rows, f32),
            pltpu.VMEM((channels, across), f32),
            pltpu.VMEM((2, channels, across), bf16),
            pltpu.VMEM((2, channels, across), bf16),
            pltpu.VMEM((4, 2, channels), f32),
            pltpu.VMEM((4, 2, channels), f32),
            pltpu.VMEM((2, 8, channels), f32),
            pltpu.VMEM((2, 8, channels), f32),
            pltpu.VMEM((2, 1, across), f32),
            pltpu.VMEM((2, 1, across), f32),
            pltpu.SemaphoreType.DMA((14,)),
            pltpu.SemaphoreType.DMA((10,)),
            pltpu.SemaphoreType.DMA((10,)),
            pltpu.SemaphoreType.REGULAR((2,)),
        ],
        compiler_params=pltpu.CompilerParams(
            collective_id=0, has_side_effects=True, vmem_limit_bytes=24 * 2**20
        ),
        cost_estimate=pl.CostEstimate(
            flops=10**9, bytes_accessed=4 * 2**20, transcendentals=0
        ),
    )(*(pltpu.with_memory_space_constraint(x, pltpu.HBM) for x in operands))
    tracers_next, cols = pl.pallas_call(
        columns_kernel,
        out_shape=(
            jax.ShapeDtypeStruct(tracers.shape, f32),
            jax.ShapeDtypeStruct((2 * features, across // 2), bf16),
        ),
        in_specs=[vmem] * 5,
        out_specs=(hbm, vmem),
        scratch_shapes=[
            pltpu.VMEM((features, columns), f32),
            pltpu.VMEM((2 * features, across // 2), f32),
            pltpu.SemaphoreType.DMA((4, 2)),
        ],
        compiler_params=pltpu.CompilerParams(vmem_limit_bytes=24 * 2**20),
    )(next_rows, start, win_t, wout_t, cost)
    return tracers_next, cols.reshape(4, levels, 2, across // 2)


def solution(mesh):
    grid = P(None, None, "grp", "bal")
    flat = P("grp", "bal")
    sizes = (mesh.shape["grp"], mesh.shape["bal"])
    return jax.shard_map(
        functools.partial(shards, sizes),
        mesh=mesh,
        in_specs=(grid, grid, flat, flat, P(), P()),
        out_specs=(grid, grid),
        check_vma=False,
    )
```

```python
import functools

import jax
import jax.numpy as jnp
import numpy as np
from jax import lax
from jax.experimental import pallas as pl
from jax.experimental.pallas import tpu as pltpu
from jax.sharding import PartitionSpec as P

MESH = pl.DeviceIdType.MESH
time_step = 0.02
remap_ints = ((9.0, 8.0, 3.0, 0.0), (0.0, 3.0, 8.0, 9.0))
gll_points = (-1.0, -0.4472135954999579, 0.4472135954999579, 1.0)

DIRS = ((1, 0), (-1, 0), (0, 1), (0, -1), (1, 1), (1, -1), (-1, 1), (-1, -1))
FROM_UP, FROM_DOWN, FROM_LEFT, FROM_RIGHT = 0, 1, 2, 3
FROM_UL, FROM_UR, FROM_DL, FROM_DR = 4, 5, 6, 7


def gll_matrix():
    points = gll_points
    matrix = np.zeros((4, 4))
    for i in range(4):
        for j in range(4):
            if i == j:
                matrix[i, i] = 2.0 * sum(
                    1.0 / (points[i] - points[k]) for k in range(4) if k != i
                )
            else:
                num = den = 1.0
                for k in range(4):
                    if k != i:
                        num *= points[i] - points[k]
                    if k != j:
                        den *= points[j] - points[k]
                matrix[i, j] = 2.0 * num / (den * (points[i] - points[j]))
    return matrix


def constants(across):
    elements, half = across // 4, across // 2
    eye = np.eye(elements)
    along = np.kron(eye, gll_matrix().T).astype(np.float32)
    high = along.astype(jnp.bfloat16)
    low = (along - high.astype(np.float32)).astype(jnp.bfloat16)
    remap = np.kron(eye, np.array(remap_ints).T).astype(jnp.bfloat16)
    pick = np.zeros((4, 8, across), np.float32)
    place = np.zeros((16, 5 * across), np.float32)
    for a in range(4):
        pick[a, a, 0] = 1.0
        pick[a, 4 + a, across - 1] = 1.0
        for part in range(2):
            place[8 * part + a, a * across] = 1.0
            place[8 * part + 4 + a, a * across + across - 1] = 1.0
            for p in range(2):
                first = 4 * across + p * half
                place[8 * part + a, first] = remap_ints[p][a] * remap_ints[0][0]
                place[8 * part + 4 + a, first + half - 1] = remap_ints[p][a] * remap_ints[1][3]
    return high, low, remap, pick.astype(jnp.bfloat16), place.astype(jnp.bfloat16)


def dot(a, b):
    return jnp.dot(a, b, preferred_element_type=jnp.float32)


def split(value):
    high = value.astype(jnp.bfloat16)
    return high, (value - high.astype(jnp.float32)).astype(jnp.bfloat16)


def kernel(
    sizes,
    tracers_hbm, winds_hbm, mass_hbm,
    dhigh_hbm, dlow_hbm, remap_hbm, pick_hbm, place_hbm, win_hbm, wout_hbm, cost_hbm,
    next_ref, start_ref, win_t_ref, wout_t_ref, cost_out_ref,
    tracers_ref, winds_ref, mass_ref,
    dhigh_ref, dlow_ref, remap_ref, pick_ref, place_ref, win_ref, wout_ref, cost_ref,
    weighted, cells_ref, rows_out, rows_in, corners_out, corners_in, sides_out, sides_in,
    mass_out, mass_in, local_sem, send_sem, recv_sem, ack_sem,
):
    n_grp, n_bal = sizes
    levels, across = winds_ref.shape[1], winds_ref.shape[3]
    grp, bal = lax.axis_index("grp"), lax.axis_index("bal")
    is_first, is_last = bal == 0, bal == n_bal - 1

    def peer(i):
        dg, db = DIRS[i]
        return (lax.rem(grp + dg + n_grp, n_grp), lax.rem(bal + db + n_bal, n_bal))

    to_left = [i for i in range(8) if DIRS[i][1] == -1]
    to_right = [i for i in range(8) if DIRS[i][1] == 1]

    def load(src, dst, slot):
        copy = pltpu.make_async_copy(src, dst, local_sem.at[slot])
        copy.start()
        return copy

    load_mass = load(mass_hbm, mass_ref, 7)
    load_rows = [load(tracers_hbm.at[:, :, a, :], tracers_ref.at[a], a) for a in range(4)]
    load_winds = load(winds_hbm, winds_ref, 6)
    load_high = load(dhigh_hbm, dhigh_ref, 4)
    load_low = load(dlow_hbm, dlow_ref, 5)
    load_pick = load(pick_hbm, pick_ref, 8)
    load_remap = load(remap_hbm, remap_ref, 9)
    load_place = load(place_hbm, place_ref, 10)

    barrier = pltpu.get_barrier_semaphore()

    def greet(i):
        pl.semaphore_signal(barrier, inc=1, device_id=peer(i), device_id_type=MESH)

    for i in range(2):
        greet(i)

    @pl.when(is_first)
    def _():
        for i in to_left:
            greet(i)

    @pl.when(jnp.logical_not(is_last))
    def _():
        for i in to_right:
            greet(i)

    load_mass.wait()

    def outermost(rows):
        return [
            jnp.broadcast_to(rows[a][:, lane : lane + 1], (1, 2 * levels))
            for lane in (0, across - 1) for a in range(4)
        ]

    own = [mass_ref[a : a + 1, :] for a in range(4)]
    mass_out[0] = own[3]
    mass_out[1] = own[0]
    mass_ends = outermost(own)
    for side in range(2):
        sides_out[side, 4:8, :] = jnp.concatenate(mass_ends[4 * side : 4 * side + 4], axis=0)
    for copy in (load_high, load_low, load_winds, *load_rows):
        copy.wait()

    def tracer_row(a):
        return tracers_ref[a].reshape(2 * levels, across)

    derivative = gll_matrix()

    def weigh(a):
        here = tracer_row(a)
        high, low = split(here)
        along_y = dot(high, dhigh_ref[...]) + dot(low, dhigh_ref[...]) + dot(high, dlow_ref[...])
        along_x = sum(float(derivative[a, c]) * tracer_row(c) for c in range(4))
        first = winds_ref[0, :, a, :].astype(jnp.float32)
        second = winds_ref[1, :, a, :].astype(jnp.float32)
        mass = mass_ref[a : a + 1, :]
        first, second = first * mass, second * mass
        for k in range(2):
            part = slice(k * levels, (k + 1) * levels)
            weighted[a, part, :] = -(first * along_x[part] + second * along_y[part])

    def picks(a, value):
        return lax.dot_general(
            pick_ref[a], value, (((1,), (1,)), ((), ())), preferred_element_type=jnp.float32
        )

    def picked(a):
        return picks(a, weighted[a].astype(jnp.bfloat16))

    for a in (0, 3):
        weigh(a)
    rows_out[0] = weighted[3].astype(jnp.bfloat16)
    rows_out[1] = weighted[0].astype(jnp.bfloat16)
    load_pick.wait()
    corners = picked(0) + picked(3)
    for c, line in enumerate((7, 3, 4, 0)):
        corners_out[c] = jnp.concatenate([corners[line : line + 1, :], mass_ends[line]], axis=0)

    def remote(src, dst, slot, i):
        return pltpu.make_async_remote_copy(
            src_ref=src, dst_ref=dst, send_sem=send_sem.at[slot], recv_sem=recv_sem.at[slot],
            device_id=peer(i), device_id_type=MESH,
        )

    mass_copies = [remote(mass_out.at[i], mass_in.at[i], i, i) for i in range(2)]
    row_copies = [remote(rows_out.at[i], rows_in.at[i], 2 + i, i) for i in range(2)]
    end_copies = {
        2: remote(sides_out.at[1], sides_in.at[0], 4, 2),
        3: remote(sides_out.at[0], sides_in.at[1], 5, 3),
        **{4 + c: remote(corners_out.at[c], corners_in.at[c], 6 + c, 4 + c) for c in range(4)},
    }

    before = jnp.where(bal > 0, 3, 0) + jnp.where(is_last, 3, 0)
    pl.semaphore_wait(barrier, 2 + before)

    def answer(slot, i):
        pl.semaphore_signal(ack_sem.at[slot], inc=1, device_id=peer(i), device_id_type=MESH)

    @pl.when(is_last)
    def _():
        for i in to_right:
            if i > 3:
                end_copies[i].start()
        for i in to_right:
            answer(0, i)

    @pl.when(jnp.logical_not(is_first))
    def _():
        for i in to_left:
            if i > 3:
                end_copies[i].start()
        for i in to_left:
            answer(1, i)

    for copy in (*mass_copies, *row_copies):
        copy.start()

    for a in (1, 2):
        weigh(a)
    ends = corners + (picked(1) + picked(2))
    for side in range(2):
        sides_out[side, 0:4, :] = ends[4 * side : 4 * side + 4, :]

    @pl.when(jnp.logical_not(is_first))
    def _():
        end_copies[3].start()

    @pl.when(is_last)
    def _():
        end_copies[2].start()

    @pl.when(jnp.logical_not(is_last))
    def _():
        pl.semaphore_wait(ack_sem.at[1], 3)
        for i in to_right:
            end_copies[i].start()

    load_win = load(win_hbm, win_ref, 11)
    load_wout = load(wout_hbm, wout_ref, 12)
    load_cost = load(cost_hbm, cost_ref, 13)

    lane = lax.broadcasted_iota(jnp.int32, (1, across), 1)
    takes_before = (lane % 4 == 0) & (lane > 0)
    takes_after = (lane % 4 == 3) & (lane < across - 1)
    inside = (lane > 0) & (lane < across - 1)

    half = across // 2
    load_remap.wait()

    def cells(mixed):
        high, low = split(mixed)
        return dot(high, remap_ref[...]) + dot(low, remap_ref[...])

    for p in range(2):
        parts = [
            sum(
                remap_ints[p][a] * winds_ref[k, :, a, :].astype(jnp.float32)
                for a in range(4) if remap_ints[p][a]
            )
            for k in range(2)
        ]
        start_ref[2 * levels :, p * half : (p + 1) * half] = (
            cells(jnp.concatenate(parts, axis=0)) * (1.0 / 400.0)
        ).astype(jnp.bfloat16)

    load_win.wait()
    win_t_ref[...] = win_ref[...].T
    load_wout.wait()
    wout_t_ref[...] = wout_ref[...].T
    load_cost.wait()
    cost_out_ref[...] = jnp.concatenate([cost_ref[0:1, :], cost_ref[1:2, :]], axis=1)

    for copy in mass_copies:
        copy.wait_recv()
    own[0] = own[0] + mass_in[FROM_UP]
    own[3] = own[3] + mass_in[FROM_DOWN]
    mass_ends = jnp.concatenate(outermost(own), axis=0)

    def joined(value):
        earlier = pltpu.roll(value, 1, 1)
        later = pltpu.roll(value, across - 1, 1)
        return value + jnp.where(takes_before, earlier, jnp.where(takes_after, later, 0.0))

    scales = [jnp.where(inside, time_step / joined(own[a]), 0.0) for a in range(4)]

    load_place.wait()

    @pl.when(is_first)
    def _():
        pl.semaphore_wait(ack_sem.at[0], 3)
        for i in to_left:
            end_copies[i].start()

    for copy in row_copies:
        copy.wait_recv()
    mixed = [None, None]
    for a in range(4):
        value = weighted[a]
        if a == 0:
            value = value + rows_in[FROM_UP].astype(jnp.float32)
        if a == 3:
            value = value + rows_in[FROM_DOWN].astype(jnp.float32)
        updated = tracer_row(a) + scales[a] * joined(value)
        next_ref[a] = updated
        for p in range(2):
            if remap_ints[p][a]:
                term = remap_ints[p][a] * updated
                mixed[p] = term if mixed[p] is None else mixed[p] + term
    ends = ends + (picks(0, rows_in[FROM_UP]) + picks(3, rows_in[FROM_DOWN]))
    for p in range(2):
        cells_ref[:, p * half : (p + 1) * half] = cells(mixed[p])

    for copy in end_copies.values():
        copy.wait_recv()

    def assembled(mine, first, line):
        none = jnp.zeros((2, 2 * levels), jnp.float32)
        upper_left, upper_right, lower_left, lower_right = (
            corners_in[i - 4, line : line + 1, :] for i in (FROM_UL, FROM_UR, FROM_DL, FROM_DR)
        )
        sides = jnp.concatenate([sides_in[side, first : first + 4, :] for side in range(2)], axis=0)
        diagonal = jnp.concatenate(
            [upper_left, none, lower_left, upper_right, none, lower_right], axis=0
        )
        return mine + (sides + diagonal)

    change = assembled(ends, 0, 0) * (time_step / assembled(mass_ends, 4, 1))
    high = change.astype(jnp.bfloat16).astype(jnp.float32)
    parts = jnp.concatenate([high, change - high], axis=0).T.astype(jnp.bfloat16)
    final = cells_ref[...] + dot(parts, place_ref[:, 4 * across :])
    start_ref[0 : 2 * levels, :] = (final * (1.0 / 400.0)).astype(jnp.bfloat16)
    for a in range(4):
        next_ref[a] = next_ref[a] + dot(parts, place_ref[:, a * across : (a + 1) * across])

    for copy in (*mass_copies, *row_copies, *end_copies.values()):
        copy.wait_send()


def doubled_gelu(value):
    inner = value * (0.7978845608028654 + 0.035677408136300125 * (value * value))
    return value + value * jnp.tanh(inner)


def columns_kernel(
    rows_ref, start_ref, win_ref, wout_ref, cost_ref, next_hbm, cols_ref, state_ref, paired_ref, store_sem
):
    levels = next_hbm.shape[1]
    stores = [
        pltpu.make_async_copy(
            rows_ref.at[a, pl.ds(k * levels, levels), :], next_hbm.at[k, :, a, :], store_sem.at[a, k]
        )
        for a in range(4) for k in range(2)
    ]
    features = win_ref.shape[1]
    half = cols_ref.shape[1]
    state_ref[...] = start_ref[...].astype(jnp.float32)

    def substep(step):
        inputs = state_ref[...].astype(jnp.bfloat16)
        hidden = doubled_gelu(dot(win_ref[...], inputs)).astype(jnp.bfloat16)
        change = dot(wout_ref[...], hidden)
        state_ref[...] += jnp.where(cost_ref[...] > step, 0.5, 0.0) * change

    for step in range(3):
        substep(step)
        if step == 0:
            for copy in stores:
                copy.start()
    current = state_ref[...]
    paired_ref[0::2, :] = current[:, :half]
    paired_ref[1::2, :] = current[:, half:]
    cols_ref[...] = paired_ref[...].astype(jnp.bfloat16)
    for copy in stores:
        copy.wait()


def shards(sizes, tracers, winds, node_mass, column_cost, weight_in, weight_out):
    levels, extent, across = tracers.shape[1:]
    features, hidden = weight_in.shape
    channels = 2 * levels
    vmem = pl.BlockSpec(memory_space=pltpu.VMEM)
    hbm = pl.BlockSpec(memory_space=pltpu.HBM)
    f32, bf16 = jnp.float32, jnp.bfloat16
    rows = (extent, channels, across)
    tables = constants(across)
    columns = column_cost.size
    operands = (tracers, winds, node_mass, *map(jnp.asarray, tables), weight_in, weight_out, column_cost)
    next_rows, start, win_t, wout_t, cost = pl.pallas_call(
        functools.partial(kernel, sizes),
        out_shape=(
            jax.ShapeDtypeStruct(rows, f32),
            jax.ShapeDtypeStruct((features, columns), bf16),
            jax.ShapeDtypeStruct((hidden, features), bf16),
            jax.ShapeDtypeStruct((features, hidden), bf16),
            jax.ShapeDtypeStruct((1, columns), column_cost.dtype),
        ),
        in_specs=[hbm] * 11,
        out_specs=(vmem,) * 5,
        scratch_shapes=[
            pltpu.VMEM((extent, 2, levels, across), f32),
            pltpu.VMEM(winds.shape, bf16),
            pltpu.VMEM(node_mass.shape, f32),
            *[pltpu.VMEM(table.shape, bf16) for table in tables],
            pltpu.VMEM(weight_in.shape, bf16),
            pltpu.VMEM(weight_out.shape, bf16),
            pltpu.VMEM(column_cost.shape, column_cost.dtype),
            pltpu.VMEM(rows, f32),
            pltpu.VMEM((channels, across), f32),
            pltpu.VMEM((2, channels, across), bf16),
            pltpu.VMEM((2, channels, across), bf16),
            pltpu.VMEM((4, 2, channels), f32),
            pltpu.VMEM((4, 2, channels), f32),
            pltpu.VMEM((2, 8, channels), f32),
            pltpu.VMEM((2, 8, channels), f32),
            pltpu.VMEM((2, 1, across), f32),
            pltpu.VMEM((2, 1, across), f32),
            pltpu.SemaphoreType.DMA((14,)),
            pltpu.SemaphoreType.DMA((10,)),
            pltpu.SemaphoreType.DMA((10,)),
            pltpu.SemaphoreType.REGULAR((2,)),
        ],
        compiler_params=pltpu.CompilerParams(
            collective_id=0, has_side_effects=True, vmem_limit_bytes=24 * 2**20
        ),
        cost_estimate=pl.CostEstimate(
            flops=10**9, bytes_accessed=4 * 2**20, transcendentals=0
        ),
    )(*(pltpu.with_memory_space_constraint(x, pltpu.HBM) for x in operands))
    tracers_next, cols = pl.pallas_call(
        columns_kernel,
        out_shape=(
            jax.ShapeDtypeStruct(tracers.shape, f32),
            jax.ShapeDtypeStruct((2 * features, across // 2), bf16),
        ),
        in_specs=[vmem] * 5,
        out_specs=(hbm, vmem),
        scratch_shapes=[
            pltpu.VMEM((features, columns), f32),
            pltpu.VMEM((2 * features, across // 2), f32),
            pltpu.SemaphoreType.DMA((4, 2)),
        ],
        compiler_params=pltpu.CompilerParams(vmem_limit_bytes=24 * 2**20),
    )(next_rows, start, win_t, wout_t, cost)
    return tracers_next, cols.reshape(4, levels, 2, across // 2)


def solution(mesh):
    grid = P(None, None, "grp", "bal")
    flat = P("grp", "bal")
    sizes = (mesh.shape["grp"], mesh.shape["bal"])
    return jax.shard_map(
        functools.partial(shards, sizes),
        mesh=mesh,
        in_specs=(grid, grid, flat, flat, P(), P()),
        out_specs=(grid, grid),
        check_vma=False,
    )
```

```python
import functools

import jax
import jax.numpy as jnp
import numpy as np
from jax import lax
from jax.experimental import pallas as pl
from jax.experimental.pallas import tpu as pltpu
from jax.sharding import PartitionSpec as P

MESH = pl.DeviceIdType.MESH
time_step = 0.02
remap_ints = ((9.0, 8.0, 3.0, 0.0), (0.0, 3.0, 8.0, 9.0))
gll_points = (-1.0, -0.4472135954999579, 0.4472135954999579, 1.0)

DIRS = ((1, 0), (-1, 0), (0, 1), (0, -1), (1, 1), (1, -1), (-1, 1), (-1, -1))
FROM_UP, FROM_DOWN, FROM_LEFT, FROM_RIGHT = 0, 1, 2, 3
FROM_UL, FROM_UR, FROM_DL, FROM_DR = 4, 5, 6, 7


def gll_matrix():
    points = gll_points
    matrix = np.zeros((4, 4))
    for i in range(4):
        for j in range(4):
            if i == j:
                matrix[i, i] = 2.0 * sum(
                    1.0 / (points[i] - points[k]) for k in range(4) if k != i
                )
            else:
                num = den = 1.0
                for k in range(4):
                    if k != i:
                        num *= points[i] - points[k]
                    if k != j:
                        den *= points[j] - points[k]
                matrix[i, j] = 2.0 * num / (den * (points[i] - points[j]))
    return matrix


def constants(across):
    elements, half = across // 4, across // 2
    eye = np.eye(elements)
    along = np.kron(eye, gll_matrix().T).astype(np.float32)
    high = along.astype(jnp.bfloat16)
    low = (along - high.astype(np.float32)).astype(jnp.bfloat16)
    remap = np.kron(eye, np.array(remap_ints).T).astype(jnp.bfloat16)
    pick = np.zeros((4, 8, across), np.float32)
    place = np.zeros((16, 5 * across), np.float32)
    for a in range(4):
        pick[a, a, 0] = 1.0
        pick[a, 4 + a, across - 1] = 1.0
        for part in range(2):
            place[8 * part + a, a * across] = 1.0
            place[8 * part + 4 + a, a * across + across - 1] = 1.0
            for p in range(2):
                first = 4 * across + p * half
                place[8 * part + a, first] = remap_ints[p][a] * remap_ints[0][0]
                place[8 * part + 4 + a, first + half - 1] = remap_ints[p][a] * remap_ints[1][3]
    return high, low, remap, pick.astype(jnp.bfloat16), place.astype(jnp.bfloat16)


def dot(a, b):
    return jnp.dot(a, b, preferred_element_type=jnp.float32)


def split(value):
    high = value.astype(jnp.bfloat16)
    return high, (value - high.astype(jnp.float32)).astype(jnp.bfloat16)


def kernel(
    sizes,
    tracers_hbm, winds_hbm, mass_hbm,
    dhigh_hbm, dlow_hbm, remap_hbm, pick_hbm, place_hbm, win_hbm, wout_hbm, cost_hbm,
    next_ref, start_ref, win_t_ref, wout_t_ref, cost_out_ref,
    tracers_ref, winds_ref, mass_ref,
    dhigh_ref, dlow_ref, remap_ref, pick_ref, place_ref, win_ref, wout_ref, cost_ref,
    weighted, cells_ref, rows_out, rows_in, corners_out, corners_in, sides_out, sides_in,
    mass_out, mass_in, local_sem, send_sem, recv_sem, ack_sem,
):
    n_grp, n_bal = sizes
    levels, across = winds_ref.shape[1], winds_ref.shape[3]
    grp, bal = lax.axis_index("grp"), lax.axis_index("bal")
    is_end = jnp.logical_or(bal == 0, bal == n_bal - 1)
    is_late = bal >= n_bal - 2

    def peer(i):
        dg, db = DIRS[i]
        return (lax.rem(grp + dg + n_grp, n_grp), lax.rem(bal + db + n_bal, n_bal))

    to_left = [i for i in range(8) if DIRS[i][1] == -1]
    to_right = [i for i in range(8) if DIRS[i][1] == 1]

    def load(src, dst, slot):
        copy = pltpu.make_async_copy(src, dst, local_sem.at[slot])
        copy.start()
        return copy

    load_mass = load(mass_hbm, mass_ref, 7)
    load_rows = [load(tracers_hbm.at[:, :, a, :], tracers_ref.at[a], a) for a in range(4)]
    load_winds = load(winds_hbm, winds_ref, 6)
    load_high = load(dhigh_hbm, dhigh_ref, 4)
    load_low = load(dlow_hbm, dlow_ref, 5)
    load_pick = load(pick_hbm, pick_ref, 8)
    load_remap = load(remap_hbm, remap_ref, 9)
    load_place = load(place_hbm, place_ref, 10)

    barrier = pltpu.get_barrier_semaphore()

    def greet(i):
        pl.semaphore_signal(barrier, inc=1, device_id=peer(i), device_id_type=MESH)

    for i in range(2):
        greet(i)

    @pl.when(is_end)
    def _():
        for i in to_left:
            greet(i)

    @pl.when(jnp.logical_not(is_late))
    def _():
        for i in to_right:
            greet(i)

    node = lax.broadcasted_iota(jnp.int32, (levels, 4 * levels), 1)
    level = lax.broadcasted_iota(jnp.int32, (levels, 4 * levels), 0)

    def selection(first, second):
        return jnp.concatenate(
            [jnp.where(node == 4 * level + a, 1.0, 0.0) for a in (first, second)], axis=0
        ).astype(jnp.bfloat16)

    load_mass.wait()

    def outermost(rows):
        return [
            jnp.broadcast_to(rows[a][:, lane : lane + 1], (1, 2 * levels))
            for lane in (0, across - 1) for a in range(4)
        ]

    own = [mass_ref[a : a + 1, :] for a in range(4)]
    mass_out[0] = own[3]
    mass_out[1] = own[0]
    mass_ends = outermost(own)
    for side in range(2):
        sides_out[side, 4:8, :] = jnp.concatenate(mass_ends[4 * side : 4 * side + 4], axis=0)
    for copy in (load_high, load_low, load_winds, *load_rows):
        copy.wait()

    def tracer_row(a):
        return tracers_ref[a].reshape(2 * levels, across)

    derivative = gll_matrix()

    def blown(first, second):
        rows = selection(first, second)
        return [dot(rows, winds_ref[k].reshape(4 * levels, across)) for k in range(2)]

    def weigh(a, winds):
        here = tracer_row(a)
        high, low = split(here)
        along_y = dot(high, dhigh_ref[...]) + dot(low, dhigh_ref[...]) + dot(high, dlow_ref[...])
        along_x = sum(float(derivative[a, c]) * tracer_row(c) for c in range(4))
        mass = -mass_ref[a : a + 1, :]
        first, second = winds[0] * mass, winds[1] * mass
        for k in range(2):
            part = slice(k * levels, (k + 1) * levels)
            weighted[a, part, :] = first * along_x[part] + second * along_y[part]

    def picks(a, value):
        return lax.dot_general(
            pick_ref[a], value, (((1,), (1,)), ((), ())), preferred_element_type=jnp.float32
        )

    def picked(a):
        return picks(a, weighted[a].astype(jnp.bfloat16))

    def weigh_pair(first, second):
        winds = blown(first, second)
        weigh(first, [wind[:levels] for wind in winds])
        weigh(second, [wind[levels:] for wind in winds])

    weigh_pair(0, 3)
    rows_out[0] = weighted[3].astype(jnp.bfloat16)
    rows_out[1] = weighted[0].astype(jnp.bfloat16)
    load_pick.wait()
    corners = picked(0) + picked(3)
    for c, line in enumerate((7, 3, 4, 0)):
        corners_out[c] = jnp.concatenate([corners[line : line + 1, :], mass_ends[line]], axis=0)

    def remote(src, dst, slot, i):
        return pltpu.make_async_remote_copy(
            src_ref=src, dst_ref=dst, send_sem=send_sem.at[slot], recv_sem=recv_sem.at[slot],
            device_id=peer(i), device_id_type=MESH,
        )

    mass_copies = [remote(mass_out.at[i], mass_in.at[i], i, i) for i in range(2)]
    row_copies = [remote(rows_out.at[i], rows_in.at[i], 2 + i, i) for i in range(2)]
    end_copies = {
        2: remote(sides_out.at[1], sides_in.at[0], 4, 2),
        3: remote(sides_out.at[0], sides_in.at[1], 5, 3),
        **{4 + c: remote(corners_out.at[c], corners_in.at[c], 6 + c, 4 + c) for c in range(4)},
    }

    before = jnp.where(bal > 0, 3, 0) + jnp.where(bal == n_bal - 2, 3, 0)
    pl.semaphore_wait(barrier, 2 + before)

    def answer(slot, i):
        pl.semaphore_signal(ack_sem.at[slot], inc=1, device_id=peer(i), device_id_type=MESH)

    @pl.when(is_late)
    def _():
        for i in to_right:
            if i > 3:
                end_copies[i].start()
        for i in to_right:
            answer(0, i)

    @pl.when(jnp.logical_not(is_end))
    def _():
        for i in to_left:
            if i > 3:
                end_copies[i].start()
        for i in to_left:
            answer(1, i)

    for copy in (*mass_copies, *row_copies):
        copy.start()

    weigh_pair(1, 2)
    ends = corners + (picked(1) + picked(2))
    for side in range(2):
        sides_out[side, 0:4, :] = ends[4 * side : 4 * side + 4, :]

    @pl.when(jnp.logical_not(is_end))
    def _():
        end_copies[3].start()

    @pl.when(is_late)
    def _():
        end_copies[2].start()

    @pl.when(jnp.logical_not(is_late))
    def _():
        pl.semaphore_wait(ack_sem.at[1], 3)
        for i in to_right:
            end_copies[i].start()

    load_win = load(win_hbm, win_ref, 11)
    load_wout = load(wout_hbm, wout_ref, 12)
    load_cost = load(cost_hbm, cost_ref, 13)

    lane = lax.broadcasted_iota(jnp.int32, (1, across), 1)
    takes_before = (lane % 4 == 0) & (lane > 0)
    takes_after = (lane % 4 == 3) & (lane < across - 1)
    inside = (lane > 0) & (lane < across - 1)

    half = across // 2
    load_remap.wait()

    def cells(mixed):
        high, low = split(mixed)
        return dot(high, remap_ref[...]) + dot(low, remap_ref[...])

    for p in range(2):
        parts = [
            sum(
                remap_ints[p][a] * winds_ref[k, :, a, :].astype(jnp.float32)
                for a in range(4) if remap_ints[p][a]
            )
            for k in range(2)
        ]
        start_ref[2 * levels :, p * half : (p + 1) * half] = (
            cells(jnp.concatenate(parts, axis=0)) * (1.0 / 400.0)
        ).astype(jnp.bfloat16)

    load_win.wait()
    win_t_ref[...] = win_ref[...].T
    load_wout.wait()
    wout_t_ref[...] = wout_ref[...].T
    load_cost.wait()
    cost_out_ref[...] = jnp.concatenate([cost_ref[0:1, :], cost_ref[1:2, :]], axis=1)

    for copy in mass_copies:
        copy.wait_recv()
    own[0] = own[0] + mass_in[FROM_UP]
    own[3] = own[3] + mass_in[FROM_DOWN]
    mass_ends = jnp.concatenate(outermost(own), axis=0)

    def joined(value):
        earlier = pltpu.roll(value, 1, 1)
        later = pltpu.roll(value, across - 1, 1)
        return value + jnp.where(takes_before, earlier, jnp.where(takes_after, later, 0.0))

    scales = [jnp.where(inside, time_step / joined(own[a]), 0.0) for a in range(4)]

    load_place.wait()

    @pl.when(is_end)
    def _():
        pl.semaphore_wait(ack_sem.at[0], 3)
        for i in to_left:
            end_copies[i].start()

    for copy in row_copies:
        copy.wait_recv()
    mixed = [None, None]
    for a in range(4):
        value = weighted[a]
        if a == 0:
            value = value + rows_in[FROM_UP].astype(jnp.float32)
        if a == 3:
            value = value + rows_in[FROM_DOWN].astype(jnp.float32)
        updated = tracer_row(a) + scales[a] * joined(value)
        next_ref[a] = updated.reshape(2, levels, across)
        for p in range(2):
            if remap_ints[p][a]:
                term = remap_ints[p][a] * updated
                mixed[p] = term if mixed[p] is None else mixed[p] + term
    ends = ends + (picks(0, rows_in[FROM_UP]) + picks(3, rows_in[FROM_DOWN]))
    for p in range(2):
        cells_ref[:, p * half : (p + 1) * half] = cells(mixed[p])

    for copy in end_copies.values():
        copy.wait_recv()

    def assembled(mine, first, line):
        none = jnp.zeros((2, 2 * levels), jnp.float32)
        upper_left, upper_right, lower_left, lower_right = (
            corners_in[i - 4, line : line + 1, :] for i in (FROM_UL, FROM_UR, FROM_DL, FROM_DR)
        )
        sides = jnp.concatenate([sides_in[side, first : first + 4, :] for side in range(2)], axis=0)
        diagonal = jnp.concatenate(
            [upper_left, none, lower_left, upper_right, none, lower_right], axis=0
        )
        return mine + (sides + diagonal)

    change = assembled(ends, 0, 0) * (time_step / assembled(mass_ends, 4, 1))
    high = change.astype(jnp.bfloat16).astype(jnp.float32)
    parts = jnp.concatenate([high, change - high], axis=0).T.astype(jnp.bfloat16)
    final = cells_ref[...] + dot(parts, place_ref[:, 4 * across :])
    start_ref[0 : 2 * levels, :] = (final * (1.0 / 400.0)).astype(jnp.bfloat16)
    for a in range(4):
        late = dot(parts, place_ref[:, a * across : (a + 1) * across])
        next_ref[a] = next_ref[a] + late.reshape(2, levels, across)

    for copy in (*mass_copies, *row_copies, *end_copies.values()):
        copy.wait_send()


def doubled_gelu(value):
    inner = value * (0.7978845608028654 + 0.035677408136300125 * (value * value))
    return value + value * jnp.tanh(inner)


def columns_kernel(
    rows_ref, start_ref, win_ref, wout_ref, cost_ref, next_hbm, cols_ref, state_ref, paired_ref, store_sem
):
    stores = [
        pltpu.make_async_copy(rows_ref.at[a], next_hbm.at[:, :, a, :], store_sem.at[a])
        for a in range(4)
    ]
    features = win_ref.shape[1]
    half = cols_ref.shape[1]
    state_ref[...] = start_ref[...].astype(jnp.float32)

    def substep(step):
        inputs = state_ref[...].astype(jnp.bfloat16)
        hidden = doubled_gelu(dot(win_ref[...], inputs)).astype(jnp.bfloat16)
        change = dot(wout_ref[...], hidden)
        state_ref[...] += jnp.where(cost_ref[...] > step, 0.5, 0.0) * change

    for step in range(3):
        substep(step)
        if step == 0:
            for copy in stores:
                copy.start()
    current = state_ref[...]
    paired_ref[0::2, :] = current[:, :half]
    paired_ref[1::2, :] = current[:, half:]
    cols_ref[...] = paired_ref[...].astype(jnp.bfloat16)
    for copy in stores:
        copy.wait()


def shards(sizes, tracers, winds, node_mass, column_cost, weight_in, weight_out):
    levels, extent, across = tracers.shape[1:]
    features, hidden = weight_in.shape
    channels = 2 * levels
    vmem = pl.BlockSpec(memory_space=pltpu.VMEM)
    hbm = pl.BlockSpec(memory_space=pltpu.HBM)
    f32, bf16 = jnp.float32, jnp.bfloat16
    rows = (extent, channels, across)
    tables = constants(across)
    columns = column_cost.size
    operands = (tracers, winds, node_mass, *map(jnp.asarray, tables), weight_in, weight_out, column_cost)
    next_rows, start, win_t, wout_t, cost = pl.pallas_call(
        functools.partial(kernel, sizes),
        out_shape=(
            jax.ShapeDtypeStruct((extent, 2, levels, across), f32),
            jax.ShapeDtypeStruct((features, columns), bf16),
            jax.ShapeDtypeStruct((hidden, features), bf16),
            jax.ShapeDtypeStruct((features, hidden), bf16),
            jax.ShapeDtypeStruct((1, columns), column_cost.dtype),
        ),
        in_specs=[hbm] * 11,
        out_specs=(vmem,) * 5,
        scratch_shapes=[
            pltpu.VMEM((extent, 2, levels, across), f32),
            pltpu.VMEM(winds.shape, bf16),
            pltpu.VMEM(node_mass.shape, f32),
            *[pltpu.VMEM(table.shape, bf16) for table in tables],
            pltpu.VMEM(weight_in.shape, bf16),
            pltpu.VMEM(weight_out.shape, bf16),
            pltpu.VMEM(column_cost.shape, column_cost.dtype),
            pltpu.VMEM(rows, f32),
            pltpu.VMEM((channels, across), f32),
            pltpu.VMEM((2, channels, across), bf16),
            pltpu.VMEM((2, channels, across), bf16),
            pltpu.VMEM((4, 2, channels), f32),
            pltpu.VMEM((4, 2, channels), f32),
            pltpu.VMEM((2, 8, channels), f32),
            pltpu.VMEM((2, 8, channels), f32),
            pltpu.VMEM((2, 1, across), f32),
            pltpu.VMEM((2, 1, across), f32),
            pltpu.SemaphoreType.DMA((14,)),
            pltpu.SemaphoreType.DMA((10,)),
            pltpu.SemaphoreType.DMA((10,)),
            pltpu.SemaphoreType.REGULAR((2,)),
        ],
        compiler_params=pltpu.CompilerParams(
            collective_id=0, has_side_effects=True, vmem_limit_bytes=24 * 2**20
        ),
        cost_estimate=pl.CostEstimate(
            flops=10**9, bytes_accessed=4 * 2**20, transcendentals=0
        ),
    )(*(pltpu.with_memory_space_constraint(x, pltpu.HBM) for x in operands))
    tracers_next, cols = pl.pallas_call(
        columns_kernel,
        out_shape=(
            jax.ShapeDtypeStruct(tracers.shape, f32),
            jax.ShapeDtypeStruct((2 * features, across // 2), bf16),
        ),
        in_specs=[vmem] * 5,
        out_specs=(hbm, vmem),
        scratch_shapes=[
            pltpu.VMEM((features, columns), f32),
            pltpu.VMEM((2 * features, across // 2), f32),
            pltpu.SemaphoreType.DMA((4,)),
        ],
        compiler_params=pltpu.CompilerParams(vmem_limit_bytes=24 * 2**20),
    )(next_rows, start, win_t, wout_t, cost)
    return tracers_next, cols.reshape(4, levels, 2, across // 2)


def solution(mesh):
    grid = P(None, None, "grp", "bal")
    flat = P("grp", "bal")
    sizes = (mesh.shape["grp"], mesh.shape["bal"])
    return jax.shard_map(
        functools.partial(shards, sizes),
        mesh=mesh,
        in_specs=(grid, grid, flat, flat, P(), P()),
        out_specs=(grid, grid),
        check_vma=False,
    )
```

```python
import functools

import jax
import jax.numpy as jnp
import numpy as np
from jax import lax
from jax.experimental import pallas as pl
from jax.experimental.pallas import tpu as pltpu
from jax.sharding import PartitionSpec as P

MESH = pl.DeviceIdType.MESH
time_step = 0.02
remap_ints = ((9.0, 8.0, 3.0, 0.0), (0.0, 3.0, 8.0, 9.0))
gll_points = (-1.0, -0.4472135954999579, 0.4472135954999579, 1.0)

DIRS = ((1, 0), (-1, 0), (0, 1), (0, -1), (1, 1), (1, -1), (-1, 1), (-1, -1))
FROM_UP, FROM_DOWN, FROM_LEFT, FROM_RIGHT = 0, 1, 2, 3
FROM_UL, FROM_UR, FROM_DL, FROM_DR = 4, 5, 6, 7


def gll_matrix():
    points = gll_points
    matrix = np.zeros((4, 4))
    for i in range(4):
        for j in range(4):
            if i == j:
                matrix[i, i] = 2.0 * sum(
                    1.0 / (points[i] - points[k]) for k in range(4) if k != i
                )
            else:
                num = den = 1.0
                for k in range(4):
                    if k != i:
                        num *= points[i] - points[k]
                    if k != j:
                        den *= points[j] - points[k]
                matrix[i, j] = 2.0 * num / (den * (points[i] - points[j]))
    return matrix


def constants(across):
    elements, half = across // 4, across // 2
    eye = np.eye(elements)
    along = np.kron(eye, gll_matrix().T).astype(np.float32)
    high = along.astype(jnp.bfloat16)
    low = (along - high.astype(np.float32)).astype(jnp.bfloat16)
    remap = np.kron(eye, np.array(remap_ints).T).astype(jnp.bfloat16)
    pick = np.zeros((4, 8, across), np.float32)
    place = np.zeros((16, 5 * across), np.float32)
    for a in range(4):
        pick[a, a, 0] = 1.0
        pick[a, 4 + a, across - 1] = 1.0
        for part in range(2):
            place[8 * part + a, a * across] = 1.0
            place[8 * part + 4 + a, a * across + across - 1] = 1.0
            for p in range(2):
                first = 4 * across + p * half
                place[8 * part + a, first] = remap_ints[p][a] * remap_ints[0][0]
                place[8 * part + 4 + a, first + half - 1] = remap_ints[p][a] * remap_ints[1][3]
    return high, low, remap, pick.astype(jnp.bfloat16), place.astype(jnp.bfloat16)


def dot(a, b):
    return jnp.dot(a, b, preferred_element_type=jnp.float32)


def split(value):
    high = value.astype(jnp.bfloat16)
    return high, (value - high.astype(jnp.float32)).astype(jnp.bfloat16)


def kernel(
    sizes,
    tracers_hbm, winds_hbm, mass_hbm,
    dhigh_hbm, dlow_hbm, remap_hbm, pick_hbm, place_hbm, win_hbm, wout_hbm, cost_hbm,
    next_ref, start_ref, win_t_ref, wout_t_ref, cost_out_ref,
    tracers_ref, winds_ref, mass_ref,
    dhigh_ref, dlow_ref, remap_ref, pick_ref, place_ref, win_ref, wout_ref, cost_ref,
    weighted, cells_ref, rows_out, rows_in, corners_out, corners_in, sides_out, sides_in,
    mass_out, mass_in, local_sem, send_sem, recv_sem, ack_sem,
):
    n_grp, n_bal = sizes
    levels, across = winds_ref.shape[1], winds_ref.shape[3]
    grp, bal = lax.axis_index("grp"), lax.axis_index("bal")
    is_end = jnp.logical_or(bal == 0, bal == n_bal - 1)
    is_late = bal >= n_bal - 2

    def peer(i):
        dg, db = DIRS[i]
        return (lax.rem(grp + dg + n_grp, n_grp), lax.rem(bal + db + n_bal, n_bal))

    to_left = [i for i in range(8) if DIRS[i][1] == -1]
    to_right = [i for i in range(8) if DIRS[i][1] == 1]

    def load(src, dst, slot):
        copy = pltpu.make_async_copy(src, dst, local_sem.at[slot])
        copy.start()
        return copy

    load_mass = load(mass_hbm, mass_ref, 7)
    load_rows = [load(tracers_hbm.at[:, :, a, :], tracers_ref.at[a], a) for a in range(4)]
    load_winds = load(winds_hbm, winds_ref, 6)
    load_high = load(dhigh_hbm, dhigh_ref, 4)
    load_low = load(dlow_hbm, dlow_ref, 5)
    load_pick = load(pick_hbm, pick_ref, 8)
    load_remap = load(remap_hbm, remap_ref, 9)
    load_place = load(place_hbm, place_ref, 10)

    barrier = pltpu.get_barrier_semaphore()

    def greet(i):
        pl.semaphore_signal(barrier, inc=1, device_id=peer(i), device_id_type=MESH)

    for i in range(2):
        greet(i)

    @pl.when(is_end)
    def _():
        for i in to_left:
            greet(i)

    @pl.when(jnp.logical_not(is_late))
    def _():
        for i in to_right:
            greet(i)

    node = lax.broadcasted_iota(jnp.int32, (levels, 4 * levels), 1)
    level = lax.broadcasted_iota(jnp.int32, (levels, 4 * levels), 0)

    def selection(first, second):
        return jnp.concatenate(
            [jnp.where(node == 4 * level + a, 1.0, 0.0) for a in (first, second)], axis=0
        ).astype(jnp.bfloat16)

    load_mass.wait()

    def outermost(rows):
        return [
            jnp.broadcast_to(rows[a][:, lane : lane + 1], (1, 2 * levels))
            for lane in (0, across - 1) for a in range(4)
        ]

    own = [mass_ref[a : a + 1, :] for a in range(4)]
    mass_out[0] = own[3]
    mass_out[1] = own[0]
    mass_ends = outermost(own)
    for side in range(2):
        sides_out[side, 4:8, :] = jnp.concatenate(mass_ends[4 * side : 4 * side + 4], axis=0)
    for copy in (load_high, load_low, load_winds, *load_rows):
        copy.wait()

    def tracer_row(a):
        return tracers_ref[a].reshape(2 * levels, across)

    derivative = gll_matrix()

    def blown(first, second):
        rows = selection(first, second)
        return [dot(rows, winds_ref[k].reshape(4 * levels, across)) for k in range(2)]

    def weigh(a, winds):
        here = tracer_row(a)
        high, low = split(here)
        along_y = dot(high, dhigh_ref[...]) + dot(low, dhigh_ref[...]) + dot(high, dlow_ref[...])
        along_x = sum(float(derivative[a, c]) * tracer_row(c) for c in range(4))
        mass = -mass_ref[a : a + 1, :]
        first, second = winds[0] * mass, winds[1] * mass
        for k in range(2):
            part = slice(k * levels, (k + 1) * levels)
            weighted[a, part, :] = first * along_x[part] + second * along_y[part]

    def picks(a, value):
        return lax.dot_general(
            pick_ref[a], value, (((1,), (1,)), ((), ())), preferred_element_type=jnp.float32
        )

    def picked(a):
        return picks(a, weighted[a].astype(jnp.bfloat16))

    def weigh_pair(first, second):
        winds = blown(first, second)
        weigh(first, [wind[:levels] for wind in winds])
        weigh(second, [wind[levels:] for wind in winds])

    weigh_pair(0, 3)
    rows_out[0] = weighted[3].astype(jnp.bfloat16)
    rows_out[1] = weighted[0].astype(jnp.bfloat16)
    load_pick.wait()
    corners = picked(0) + picked(3)
    for c, line in enumerate((7, 3, 4, 0)):
        corners_out[c] = jnp.concatenate([corners[line : line + 1, :], mass_ends[line]], axis=0)

    def remote(src, dst, slot, i):
        return pltpu.make_async_remote_copy(
            src_ref=src, dst_ref=dst, send_sem=send_sem.at[slot], recv_sem=recv_sem.at[slot],
            device_id=peer(i), device_id_type=MESH,
        )

    mass_copies = [remote(mass_out.at[i], mass_in.at[i], i, i) for i in range(2)]
    row_copies = [remote(rows_out.at[i], rows_in.at[i], 2 + i, i) for i in range(2)]
    end_copies = {
        2: remote(sides_out.at[1], sides_in.at[0], 4, 2),
        3: remote(sides_out.at[0], sides_in.at[1], 5, 3),
        **{4 + c: remote(corners_out.at[c], corners_in.at[c], 6 + c, 4 + c) for c in range(4)},
    }

    before = jnp.where(bal > 0, 3, 0) + jnp.where(bal == n_bal - 2, 3, 0)
    pl.semaphore_wait(barrier, 2 + before)

    def answer(slot, i):
        pl.semaphore_signal(ack_sem.at[slot], inc=1, device_id=peer(i), device_id_type=MESH)

    @pl.when(is_late)
    def _():
        for i in to_right:
            if i > 3:
                end_copies[i].start()
        for i in to_right:
            answer(0, i)

    @pl.when(jnp.logical_not(is_end))
    def _():
        for i in to_left:
            if i > 3:
                end_copies[i].start()
        for i in to_left:
            answer(1, i)

    for copy in (*row_copies, *mass_copies):
        copy.start()

    weigh_pair(1, 2)
    ends = corners + (picked(1) + picked(2))
    for side in range(2):
        sides_out[side, 0:4, :] = ends[4 * side : 4 * side + 4, :]

    @pl.when(jnp.logical_not(is_end))
    def _():
        end_copies[3].start()

    @pl.when(is_late)
    def _():
        end_copies[2].start()

    @pl.when(jnp.logical_not(is_late))
    def _():
        pl.semaphore_wait(ack_sem.at[1], 3)
        for i in to_right:
            end_copies[i].start()

    load_win = load(win_hbm, win_ref, 11)
    load_wout = load(wout_hbm, wout_ref, 12)
    load_cost = load(cost_hbm, cost_ref, 13)

    lane = lax.broadcasted_iota(jnp.int32, (1, across), 1)
    takes_before = (lane % 4 == 0) & (lane > 0)
    takes_after = (lane % 4 == 3) & (lane < across - 1)
    inside = (lane > 0) & (lane < across - 1)

    half = across // 2
    load_remap.wait()

    def cells(mixed):
        high, low = split(mixed)
        return dot(high, remap_ref[...]) + dot(low, remap_ref[...])

    for p in range(2):
        parts = [
            sum(
                remap_ints[p][a] * winds_ref[k, :, a, :].astype(jnp.float32)
                for a in range(4) if remap_ints[p][a]
            )
            for k in range(2)
        ]
        start_ref[2 * levels :, p * half : (p + 1) * half] = (
            cells(jnp.concatenate(parts, axis=0)) * (1.0 / 400.0)
        ).astype(jnp.bfloat16)

    load_win.wait()
    win_t_ref[...] = win_ref[...].T
    load_wout.wait()
    wout_t_ref[...] = wout_ref[...].T
    load_cost.wait()
    cost_out_ref[...] = jnp.concatenate([cost_ref[0:1, :], cost_ref[1:2, :]], axis=1)

    for copy in mass_copies:
        copy.wait_recv()
    own[0] = own[0] + mass_in[FROM_UP]
    own[3] = own[3] + mass_in[FROM_DOWN]
    mass_ends = jnp.concatenate(outermost(own), axis=0)

    def joined(value):
        earlier = pltpu.roll(value, 1, 1)
        later = pltpu.roll(value, across - 1, 1)
        return value + jnp.where(takes_before, earlier, jnp.where(takes_after, later, 0.0))

    scales = [jnp.where(inside, time_step / joined(own[a]), 0.0) for a in range(4)]

    load_place.wait()

    @pl.when(is_end)
    def _():
        pl.semaphore_wait(ack_sem.at[0], 3)
        for i in to_left:
            end_copies[i].start()

    for copy in row_copies:
        copy.wait_recv()
    mixed = [None, None]
    for a in range(4):
        value = weighted[a]
        if a == 0:
            value = value + rows_in[FROM_UP].astype(jnp.float32)
        if a == 3:
            value = value + rows_in[FROM_DOWN].astype(jnp.float32)
        updated = tracer_row(a) + scales[a] * joined(value)
        next_ref[a] = updated.reshape(2, levels, across)
        for p in range(2):
            if remap_ints[p][a]:
                term = remap_ints[p][a] * updated
                mixed[p] = term if mixed[p] is None else mixed[p] + term
    ends = ends + (picks(0, rows_in[FROM_UP]) + picks(3, rows_in[FROM_DOWN]))
    for p in range(2):
        cells_ref[:, p * half : (p + 1) * half] = cells(mixed[p])

    for copy in end_copies.values():
        copy.wait_recv()

    def assembled(mine, first, line):
        none = jnp.zeros((2, 2 * levels), jnp.float32)
        upper_left, upper_right, lower_left, lower_right = (
            corners_in[i - 4, line : line + 1, :] for i in (FROM_UL, FROM_UR, FROM_DL, FROM_DR)
        )
        sides = jnp.concatenate([sides_in[side, first : first + 4, :] for side in range(2)], axis=0)
        diagonal = jnp.concatenate(
            [upper_left, none, lower_left, upper_right, none, lower_right], axis=0
        )
        return mine + (sides + diagonal)

    change = assembled(ends, 0, 0) * (time_step / assembled(mass_ends, 4, 1))
    high = change.astype(jnp.bfloat16).astype(jnp.float32)
    parts = jnp.concatenate([high, change - high], axis=0).T.astype(jnp.bfloat16)
    final = cells_ref[...] + dot(parts, place_ref[:, 4 * across :])
    start_ref[0 : 2 * levels, :] = (final * (1.0 / 400.0)).astype(jnp.bfloat16)
    for a in range(4):
        late = dot(parts, place_ref[:, a * across : (a + 1) * across])
        next_ref[a] = next_ref[a] + late.reshape(2, levels, across)

    for copy in (*mass_copies, *row_copies, *end_copies.values()):
        copy.wait_send()


def doubled_gelu(value):
    inner = value * (0.7978845608028654 + 0.035677408136300125 * (value * value))
    return value + value * jnp.tanh(inner)


def columns_kernel(
    rows_ref, start_ref, win_ref, wout_ref, cost_ref, next_hbm, cols_ref, state_ref, paired_ref, store_sem
):
    stores = [
        pltpu.make_async_copy(rows_ref.at[a], next_hbm.at[:, :, a, :], store_sem.at[a])
        for a in range(4)
    ]
    features = win_ref.shape[1]
    half = cols_ref.shape[1]
    state_ref[...] = start_ref[...].astype(jnp.float32)

    def substep(step):
        inputs = state_ref[...].astype(jnp.bfloat16)
        hidden = doubled_gelu(dot(win_ref[...], inputs)).astype(jnp.bfloat16)
        change = dot(wout_ref[...], hidden)
        state_ref[...] += jnp.where(cost_ref[...] > step, 0.5, 0.0) * change

    for step in range(3):
        substep(step)
        if step == 0:
            for copy in stores:
                copy.start()
    current = state_ref[...]
    paired_ref[0::2, :] = current[:, :half]
    paired_ref[1::2, :] = current[:, half:]
    cols_ref[...] = paired_ref[...].astype(jnp.bfloat16)
    for copy in stores:
        copy.wait()


def shards(sizes, tracers, winds, node_mass, column_cost, weight_in, weight_out):
    levels, extent, across = tracers.shape[1:]
    features, hidden = weight_in.shape
    channels = 2 * levels
    vmem = pl.BlockSpec(memory_space=pltpu.VMEM)
    hbm = pl.BlockSpec(memory_space=pltpu.HBM)
    f32, bf16 = jnp.float32, jnp.bfloat16
    rows = (extent, channels, across)
    tables = constants(across)
    columns = column_cost.size
    operands = (tracers, winds, node_mass, *map(jnp.asarray, tables), weight_in, weight_out, column_cost)
    next_rows, start, win_t, wout_t, cost = pl.pallas_call(
        functools.partial(kernel, sizes),
        out_shape=(
            jax.ShapeDtypeStruct((extent, 2, levels, across), f32),
            jax.ShapeDtypeStruct((features, columns), bf16),
            jax.ShapeDtypeStruct((hidden, features), bf16),
            jax.ShapeDtypeStruct((features, hidden), bf16),
            jax.ShapeDtypeStruct((1, columns), column_cost.dtype),
        ),
        in_specs=[hbm] * 11,
        out_specs=(vmem,) * 5,
        scratch_shapes=[
            pltpu.VMEM((extent, 2, levels, across), f32),
            pltpu.VMEM(winds.shape, bf16),
            pltpu.VMEM(node_mass.shape, f32),
            *[pltpu.VMEM(table.shape, bf16) for table in tables],
            pltpu.VMEM(weight_in.shape, bf16),
            pltpu.VMEM(weight_out.shape, bf16),
            pltpu.VMEM(column_cost.shape, column_cost.dtype),
            pltpu.VMEM(rows, f32),
            pltpu.VMEM((channels, across), f32),
            pltpu.VMEM((2, channels, across), bf16),
            pltpu.VMEM((2, channels, across), bf16),
            pltpu.VMEM((4, 2, channels), f32),
            pltpu.VMEM((4, 2, channels), f32),
            pltpu.VMEM((2, 8, channels), f32),
            pltpu.VMEM((2, 8, channels), f32),
            pltpu.VMEM((2, 1, across), f32),
            pltpu.VMEM((2, 1, across), f32),
            pltpu.SemaphoreType.DMA((14,)),
            pltpu.SemaphoreType.DMA((10,)),
            pltpu.SemaphoreType.DMA((10,)),
            pltpu.SemaphoreType.REGULAR((2,)),
        ],
        compiler_params=pltpu.CompilerParams(
            collective_id=0, has_side_effects=True, vmem_limit_bytes=24 * 2**20
        ),
        cost_estimate=pl.CostEstimate(
            flops=10**9, bytes_accessed=4 * 2**20, transcendentals=0
        ),
    )(*(pltpu.with_memory_space_constraint(x, pltpu.HBM) for x in operands))
    tracers_next, cols = pl.pallas_call(
        columns_kernel,
        out_shape=(
            jax.ShapeDtypeStruct(tracers.shape, f32),
            jax.ShapeDtypeStruct((2 * features, across // 2), bf16),
        ),
        in_specs=[vmem] * 5,
        out_specs=(hbm, vmem),
        scratch_shapes=[
            pltpu.VMEM((features, columns), f32),
            pltpu.VMEM((2 * features, across // 2), f32),
            pltpu.SemaphoreType.DMA((4,)),
        ],
        compiler_params=pltpu.CompilerParams(vmem_limit_bytes=24 * 2**20),
    )(next_rows, start, win_t, wout_t, cost)
    return tracers_next, cols.reshape(4, levels, 2, across // 2)


def solution(mesh):
    grid = P(None, None, "grp", "bal")
    flat = P("grp", "bal")
    sizes = (mesh.shape["grp"], mesh.shape["bal"])
    return jax.shard_map(
        functools.partial(shards, sizes),
        mesh=mesh,
        in_specs=(grid, grid, flat, flat, P(), P()),
        out_specs=(grid, grid),
        check_vma=False,
    )
```
